32 devices in a mesh: group: 2 (over y), seq: 16 (over z, x, core).
Axes of the slice: x: 2, y: 2, z: 4, core: 2. Of those that a mesh axis runs over, the one named last changes fastest.
Arguments:
- tiles: bfloat16 [2, 6144, 1536], P('group', 'seq'), may hold values from -6 to 6
- tile_counts: int32 [2, 16], P('group', 'seq'), may hold values from 1 to 352, as said below
- w_gate: bfloat16 [1536, 2048], P(None, ('group', 'seq')), may hold values from -0.15625 to 0.15625
- w_up: bfloat16 [1536, 2048], P(None, ('group', 'seq')), may hold values from -0.15625 to 0.15625
- w_down_t: bfloat16 [1536, 2048], P(None, ('group', 'seq')), may hold values from -0.125 to 0.125
- w_embed: bfloat16 [1536, 768], replicated, may hold values from -0.15625 to 0.15625
- w_query: bfloat16 [768, 768], replicated, may hold values from -2 to 2
- w_key: bfloat16 [768, 768], replicated, may hold values from -2 to 2
- w_value: bfloat16 [768, 768], replicated, may hold values from -0.21875 to 0.21875
- w_out: bfloat16 [768, 768], replicated, may hold values from -0.21875 to 0.21875
- cotangent: bfloat16 [2, 6144, 768], P('group', 'seq'), may hold values from -6 to 6
Outputs:
- slide_out: bfloat16 [2, 6144, 768], P('group', 'seq')
- grad_value: float32 [768, 768], P('seq')
- grad_out: float32 [768, 768], P('seq')
The draws below stay inside these ranges and needn't reach their ends.
Inputs may be any that keep to these rules, and one draw needn't show every extreme that they name: `tile_counts`: the counts of slides 2i and 2i+1 at the same block index, each rounded up to whole blocks of 32 tiles, add up to at most 12 blocks; in every draw some pair reaches that. The tissue tiles of a block are its first positions.
All inputs are finite; a program needn't handle non-finite values.
Results may differ from the reference program's by a relative error of at most 0.03.
Values may be sent and summed in bfloat16 or wider, within the bound.
No kernel may reach another device: no remote copies, remote signals or barrier semaphores. Data moves between devices by JAX's collectives and lax.ppermute only.
A program may use at most 128 MiB of HBM per device.

```python
import math
import jax
import jax.numpy as jnp
from jax import lax

D = 1536
FF_WIN = 2048
E = 768
HEADS = 16
HEAD = 48
TOK_DEV = 384
RATE = 16
BLOCK = 32
SLIDES = 2
TOKENS = 6144
GLOBAL = 384
N_SEQ = 16


def draw_tile_counts(key, part):
    pairs = SLIDES // 2
    per_device = TOK_DEV // BLOCK
    half_blocks = per_device // 2
    key_side, key_dense, key_sparse = jax.random.split(jax.random.fold_in(key, 17), 3)
    dense_side = jax.random.randint(key_side, (pairs, 1), 0, 2)
    dense_rows = jax.random.randint(key_dense, (pairs, N_SEQ), half_blocks * BLOCK + 1, (per_device - 1) * BLOCK + 1)
    dense_rows = dense_rows.at[0, 0].set((per_device - 1) * BLOCK)
    dense_blocks = (dense_rows + BLOCK - 1) // BLOCK
    spare_rows = (per_device - dense_blocks) * BLOCK
    sparse_rows = 1 + jax.random.randint(key_sparse, (pairs, N_SEQ), 0, 1 << 20) % spare_rows
    sparse_rows = sparse_rows.at[0, 0].set(spare_rows[0, 0])
    first_slide = jnp.where(dense_side == 1, dense_rows, sparse_rows)
    second_slide = jnp.where(dense_side == 1, sparse_rows, dense_rows)
    return jnp.stack([first_slide, second_slide], axis=1).reshape(SLIDES, N_SEQ).astype(jnp.int32)


def query_key_pair(key):
    base_key = jax.random.fold_in(key, 31)
    shared = jax.random.normal(jax.random.fold_in(base_key, 1), (E, E), jnp.float32) / math.sqrt(E)
    other_draw = jax.random.normal(jax.random.fold_in(base_key, 2), (E, E), jnp.float32) / math.sqrt(E)
    query_part = shared
    key_part = other_draw
    return (jnp.clip(query_part, -2.0, 2.0), jnp.clip(key_part, -2.0, 2.0))


def draw_w_query(key, part):
    return query_key_pair(key)[0].astype(jnp.bfloat16)


def draw_w_key(key, part):
    return query_key_pair(key)[1].astype(jnp.bfloat16)


def level_of(own_key, extent, cuts, smallest, largest):
    def one(axis_at, parts):
        heights = jax.random.uniform(jax.random.fold_in(jax.random.fold_in(own_key, 6), axis_at), (parts,), jnp.float32, smallest / len(cuts), largest / len(cuts))
        return jnp.repeat(jnp.exp(heights), extent[axis_at] // parts).reshape((-1,) + (1,) * (len(extent) - axis_at - 1))

    factor_of = one(*cuts[0])
    for cut in cuts[1:]:
        factor_of = factor_of * one(*cut)
    return factor_of


def gaussian(rng, extent, scale, reach, cuts=(), held_as=jnp.bfloat16):
    entries = jax.random.normal(rng, extent, jnp.float32) * scale
    if len(cuts) > 0:
        entries = level_of(rng, extent, cuts, -0.22, 0.18) * entries
    return jnp.clip(entries, min=-reach, max=reach).astype(held_as)


def setup_inputs(seed: int = 0) -> dict:
    arg_keys = jax.random.split(jax.random.key(seed), 12)
    return {
        "tiles": gaussian(arg_keys[0], (SLIDES, TOKENS, D), 1.0, 6.0, ((0, 2), (1, 16))),
        "tile_counts": draw_tile_counts(jax.random.fold_in(arg_keys[11], 71), 0),
        "w_gate": gaussian(arg_keys[2], (D, FF_WIN), D ** -0.5, 0.15625, ((1, 32),)),
        "w_up": gaussian(arg_keys[3], (D, FF_WIN), D ** -0.5, 0.15625, ((1, 32),)),
        "w_down_t": gaussian(arg_keys[4], (D, FF_WIN), FF_WIN ** -0.5, 0.125, ((1, 32),)),
        "w_embed": gaussian(arg_keys[5], (D, E), D ** -0.5, 0.15625),
        "w_query": draw_w_query(jax.random.fold_in(arg_keys[11], 71), 0),
        "w_key": draw_w_key(jax.random.fold_in(arg_keys[11], 71), 0),
        "w_value": gaussian(arg_keys[8], (E, E), E ** -0.5, 0.21875),
        "w_out": gaussian(arg_keys[9], (E, E), E ** -0.5, 0.21875),
        "cotangent": gaussian(arg_keys[10], (SLIDES, TOKENS, E), 1.0, 6.0, ((0, 2), (1, 16))),
    }


def rms_rows(values):
    values = values.astype(jnp.float32)
    return values * lax.rsqrt(lax.optimization_barrier(jnp.mean(values * values, axis=-1, keepdims=True)) + 1e-06)

def project(left, right):
    return jnp.dot(left, right, preferred_element_type=jnp.float32)

def reference(tiles, tile_counts, w_gate, w_up, w_down_t, w_embed, w_query, w_key, w_value, w_out, cotangent):
    score_scale = 1.0 / math.sqrt(HEAD)
    highest = lax.Precision.HIGHEST

    def one_slide(running, slide_in):
        tile_rows, slide_counts, grad_in = slide_in
        normed = rms_rows(tile_rows).astype(jnp.bfloat16)
        active = (jax.nn.silu(project(normed, w_gate)) * project(normed, w_up)).astype(jnp.bfloat16)
        encoded = tile_rows.astype(jnp.float32) + project(active, w_down_t.T)
        embedded = rms_rows(encoded).astype(jnp.bfloat16)
        slide_tok = project(embedded, w_embed).astype(jnp.bfloat16)
        slide_normed = rms_rows(slide_tok).astype(jnp.bfloat16)
        queries = project(slide_normed, w_query).astype(jnp.bfloat16)
        key_rows = project(slide_normed, w_key).astype(jnp.bfloat16)
        value_rows = project(slide_normed, w_value).astype(jnp.bfloat16)
        positions = jnp.arange(TOKENS, dtype=jnp.int32)
        is_valid = positions % TOK_DEV < jnp.repeat(slide_counts, TOK_DEV)
        grad_y = jnp.where(is_valid[:, None], grad_in, jnp.zeros_like(grad_in))
        far_keys = key_rows[::RATE].astype(jnp.float32).reshape(-1, HEADS, HEAD)
        far_values = value_rows[::RATE].astype(jnp.float32).reshape(-1, HEADS, HEAD)
        far_valid = is_valid[::RATE]

        def one_block(far_sum, block_in):
            query_block, key_block, value_block, valid_block, slide_block, grady_block = block_in
            key_set = jnp.concatenate([key_block.astype(jnp.float32).reshape(-1, HEADS, HEAD), far_keys], axis=0)
            value_set = jnp.concatenate([value_block.astype(jnp.float32).reshape(-1, HEADS, HEAD), far_values], axis=0)
            key_valid = jnp.concatenate([valid_block, far_valid])
            query_heads = query_block.astype(jnp.float32).reshape(-1, HEADS, HEAD)
            scores = jnp.einsum('phd,jhd->hpj', query_heads, key_set, precision=highest) * score_scale
            scores = jnp.where(key_valid[None, None, :], scores, -1e+30)
            row_max = lax.optimization_barrier(jnp.max(scores, axis=2, keepdims=True))
            exponent = jnp.exp(scores - row_max)
            weights = (exponent / lax.optimization_barrier(jnp.sum(exponent, axis=2, keepdims=True))).astype(jnp.bfloat16)
            weights_f = weights.astype(jnp.float32)
            attended = jnp.einsum('hpj,jhd->phd', weights_f, value_set, precision=highest)
            attended = attended.reshape(TOK_DEV, E).astype(jnp.bfloat16)
            output = slide_block.astype(jnp.float32) + project(attended, w_out)
            out_block = jnp.where(valid_block[:, None], output, 0.0).astype(jnp.bfloat16)
            grad_att = project(grady_block, w_out.T).astype(jnp.bfloat16)
            grad_heads = grad_att.astype(jnp.float32).reshape(TOK_DEV, HEADS, HEAD)
            local_grad = jnp.einsum('hpj,phd->jhd', weights_f[:, :, :TOK_DEV], grad_heads, precision=highest)
            far_part = jnp.einsum('hpj,phd->jhd', weights_f[:, :, TOK_DEV:], grad_heads, precision=highest)
            return (far_sum + far_part.reshape(-1, E), (out_block, attended, local_grad.reshape(TOK_DEV, E)))
        blocks = (queries.reshape(N_SEQ, TOK_DEV, E), key_rows.reshape(N_SEQ, TOK_DEV, E), value_rows.reshape(N_SEQ, TOK_DEV, E), is_valid.reshape(N_SEQ, TOK_DEV), slide_tok.reshape(N_SEQ, TOK_DEV, E), grad_y.reshape(N_SEQ, TOK_DEV, E))
        far_sum, (outs, attended, local_grad) = lax.scan(one_block, jnp.zeros((GLOBAL, E), jnp.float32), blocks)
        grad_values = local_grad.reshape(TOKENS, E).at[::RATE].add(far_sum).astype(jnp.bfloat16)
        grad_value = running[0] + project(slide_normed.T, grad_values)
        grad_out = running[1] + project(attended.reshape(TOKENS, E).T, grad_y)
        return ((grad_value, grad_out), outs.reshape(TOKENS, E))
    zeros_square = jnp.zeros((E, E), jnp.float32)
    (grad_value, grad_out), slide_out = lax.scan(one_slide, (zeros_square, zeros_square), (tiles, tile_counts, cotangent))
    return (slide_out, grad_value, grad_out)
```

```python
import math

import jax
import jax.numpy as jnp
from jax import lax
from jax.sharding import PartitionSpec as P

HEADS = 16
HEAD = 48
RATE = 16
BLOCK = 32

epsilon = 1e-06
BOTH = ("group", "seq")


def rms_rows(values):
    values = values.astype(jnp.float32)
    return values * lax.rsqrt(jnp.mean(values * values, axis=-1, keepdims=True) + epsilon)


def mm(left, right):
    return jnp.dot(left, right, preferred_element_type=jnp.float32)


def mm_nt(left, right):
    return lax.dot_general(
        left, right, (((1,), (1,)), ((), ())), preferred_element_type=jnp.float32
    )


def mm_tn(left, right):
    return lax.dot_general(
        left, right, (((0,), (0,)), ((), ())), preferred_element_type=jnp.float32
    )


class Moves:
    def __init__(self, groups, seqs):
        self.groups, self.seqs = groups, seqs
        self.rests = seqs // 4
        self.ring = (groups // 2) * self.rests

    def seq_xor(self, value, bit):
        return lax.ppermute(value, "seq", [(s, s ^ bit) for s in range(self.seqs)])

    def core(self, value):
        return self.seq_xor(value, 1)

    def x(self, value):
        return self.seq_xor(value, 2)

    def y(self, value):
        return lax.ppermute(value, "group", [(g, g ^ 1) for g in range(self.groups)])

    def rest_shift(self, value, step):
        pairs = []
        for s in range(self.seqs):
            target = ((s // 4 + step) % self.rests) * 4 + s % 4
            pairs.append((s, target))
        return lax.ppermute(value, "seq", pairs)

    def ring_next(self, value):
        pairs = []
        for g in range(self.groups):
            for s in range(self.seqs):
                place = ((g // 2) * self.rests + s // 4 + 1) % self.ring
                to_g = (place // self.rests) * 2 + g % 2
                to_s = (place % self.rests) * 4 + s % 4
                pairs.append((g * self.seqs + s, to_g * self.seqs + to_s))
        return lax.ppermute(value, BOTH, pairs)


def take(array, index, axis):
    return lax.dynamic_index_in_dim(array, index, axis, keepdims=False)


def ffn_term(rows, chunks, hidden):
    gate = jnp.concatenate([c[:hidden] for c in chunks], axis=0)
    upward = jnp.concatenate([c[hidden : 2 * hidden] for c in chunks], axis=0)
    down = jnp.concatenate([c[2 * hidden :] for c in chunks], axis=0)
    active = (jax.nn.silu(mm_nt(rows, gate)) * mm_nt(rows, upward)).astype(jnp.bfloat16)
    return mm(active, down)


def flip_blocks(rows):
    width = rows.shape[1]
    return rows.reshape(-1, BLOCK, width)[::-1].reshape(-1, width)


def encode(moves, tile_rows, row_count, w_gate, w_up, w_down_t, w_embed):
    hidden = w_gate.shape[1]
    half = tile_rows.shape[0] // 2
    spare = half - BLOCK
    chunk = jnp.concatenate([w_gate.T, w_up.T, w_down_t.T], axis=0)
    ringed = [chunk]
    for _ in range(moves.ring - 1):
        ringed.append(moves.ring_next(ringed[-1]))
    chunks = [[c, moves.core(c)] for c in ringed]
    extra = moves.y(flip_blocks(tile_rows[half : half + spare]))
    own_blocks = (row_count + BLOCK - 1) // BLOCK
    kept = (1 + jnp.arange(spare) // BLOCK) < own_blocks
    level = jnp.concatenate(
        [tile_rows[:BLOCK], jnp.where(kept[:, None], tile_rows[BLOCK:half], extra)], axis=0
    )
    normed = rms_rows(level).astype(jnp.bfloat16)
    part = half // 2
    first, second = normed[:part], normed[part:]
    first = jnp.concatenate([first, moves.x(first)], axis=0)
    second = jnp.concatenate([second, moves.y(second)], axis=0)
    rows = jnp.concatenate([first, second, moves.y(first), moves.x(second)], axis=0)
    early = [c for pair in chunks[:-1] for c in pair]
    mixed = ffn_term(rows, chunks[-1], hidden)
    if early:
        mixed = mixed + ffn_term(rows, early, hidden)
    low = mixed.astype(jnp.bfloat16)
    first = mixed[: 2 * part] + moves.y(low[4 * part : 6 * part]).astype(jnp.float32)
    second = mixed[2 * part : 4 * part] + moves.x(low[6 * part :]).astype(jnp.float32)
    first = first[:part] + moves.x(first[part:].astype(jnp.bfloat16)).astype(jnp.float32)
    second = second[:part] + moves.y(second[part:].astype(jnp.bfloat16)).astype(jnp.float32)
    mixed = jnp.concatenate([first, second], axis=0)
    embedded = rms_rows(level.astype(jnp.float32) + mixed).astype(jnp.bfloat16)
    slide_part = mm(embedded, w_embed).astype(jnp.bfloat16)
    back = moves.y(flip_blocks(slide_part[BLOCK:]))
    return jnp.concatenate([slide_part, back], axis=0)


def reduce_grads(moves, part_value, part_out):
    seqs = moves.seqs
    features, width = part_value.shape
    seq_index, group_index = lax.axis_index("seq"), lax.axis_index("group")
    core_bit, x_bit, rest = seq_index % 2, (seq_index // 2) % 2, seq_index // 4
    y_bit = group_index % 2
    share = features // seqs // 2
    low = jnp.bfloat16

    def halve(array, bit, axis, move):
        kept = take(array, bit, axis).astype(jnp.float32)
        return kept + move(take(array, 1 - bit, axis).astype(low)).astype(jnp.float32)

    def split(array):
        return array.reshape(moves.rests, 2, 2, 2, share, width)

    value = halve(split(part_value), core_bit, 2, moves.core)
    out = halve(split(part_out), core_bit, 2, moves.core)
    value = halve(value, x_bit, 1, moves.x)
    out = halve(out, y_bit, 2, moves.y)
    value = halve(value, y_bit, 1, moves.y)
    out = halve(out, x_bit, 1, moves.x)
    both = jnp.concatenate([value, out], axis=2)
    total = take(both, rest, 0)
    sent = both.astype(low)
    for step in range(1, moves.rests):
        block = take(sent, (rest + step) % moves.rests, 0)
        total = total + moves.rest_shift(block, step).astype(jnp.float32)
    total = total.astype(low)
    if moves.groups > 2:
        fellows = [list(range(bit, moves.groups, 2)) for bit in range(2)]
        everyone = lax.all_gather(total, "group", axis=0, axis_index_groups=fellows)
        total = jnp.sum(everyone.astype(jnp.float32), axis=0).astype(low)
    other = moves.y(total)
    top = jnp.where(y_bit == 0, total, other)
    bottom = jnp.where(y_bit == 0, other, total)
    full = jnp.concatenate([top, bottom], axis=0).astype(jnp.float32)
    return full[:, :width], full[:, width:]


def gather_far(moves, block):
    bit = moves.seqs // 2
    while bit >= 1:
        block = jnp.concatenate([block, moves.seq_xor(block, bit)], axis=0)
        bit //= 2
    return block


def shards(
    tiles, tile_counts, w_gate, w_up, w_down_t, w_embed, w_query, w_key, w_value, w_out, cotangent
):
    moves = Moves(lax.axis_size("group"), lax.axis_size("seq"))
    tile_rows = tiles[0]
    row_count = tile_counts[0, 0]
    seq_len = tile_rows.shape[0]
    live = seq_len - BLOCK
    is_valid = jnp.arange(live) < row_count
    grad_y = jnp.where(is_valid[:, None], cotangent[0, :live], jnp.zeros((), cotangent.dtype))
    grad_att = mm_nt(grad_y, w_out).astype(jnp.bfloat16)

    slide_tok = encode(moves, tile_rows, row_count, w_gate, w_up, w_down_t, w_embed)
    score_scale = 1.0 / math.sqrt(HEAD)
    slide_normed = rms_rows(slide_tok).astype(jnp.bfloat16)
    width = slide_normed.shape[1]
    dilated = seq_len // RATE
    held = live // RATE
    far_count = ((row_count + RATE - 1) // RATE).astype(jnp.bfloat16)
    far_rows = gather_far(
        moves,
        jnp.concatenate(
            [
                slide_normed.reshape(held, RATE, width)[:, 0],
                jnp.full((dilated - held, width), far_count, jnp.bfloat16),
            ],
            axis=0,
        ),
    )
    far_blocks = far_rows.reshape(moves.seqs, dilated, width)
    far_valid = (
        jnp.arange(dilated)[None, :] < far_blocks[:, dilated - 1, :1].astype(jnp.float32)
    ).reshape(-1)
    queries = mm(slide_normed, w_query).astype(jnp.bfloat16)
    all_rows = jnp.concatenate([slide_normed, far_rows], axis=0)
    key_set = mm(all_rows, w_key).astype(jnp.bfloat16).reshape(-1, HEADS, HEAD)
    value_set = mm(all_rows, w_value).astype(jnp.bfloat16).reshape(-1, HEADS, HEAD)
    key_valid = jnp.concatenate([is_valid, far_valid])
    query_heads = queries.reshape(live, HEADS, HEAD)
    scores = (
        jnp.einsum("phd,jhd->hpj", query_heads, key_set, preferred_element_type=jnp.float32)
        * score_scale
    )
    scores = jnp.where(key_valid[None, None, :], scores, -1e30)
    row_max = jnp.max(scores, axis=2, keepdims=True)
    exponent = jnp.exp(scores - row_max)
    weights = (exponent / jnp.sum(exponent, axis=2, keepdims=True)).astype(jnp.bfloat16)
    attended = jnp.einsum("hpj,jhd->phd", weights, value_set, preferred_element_type=jnp.float32)
    attended = attended.reshape(live, width).astype(jnp.bfloat16)
    output = slide_tok.astype(jnp.float32) + mm(attended, w_out)
    slide_out = jnp.where(is_valid[:, None], output, 0.0).astype(jnp.bfloat16)
    slide_out = jnp.concatenate([slide_out, jnp.zeros((BLOCK, width), jnp.bfloat16)], axis=0)
    part_out = mm_tn(attended, grad_y)
    grad_heads = grad_att.reshape(live, HEADS, HEAD)
    grad_values = jnp.einsum(
        "hpj,phd->jhd", weights, grad_heads, preferred_element_type=jnp.float32
    )
    grad_values = grad_values.reshape(-1, width).astype(jnp.bfloat16)
    part_value = mm_tn(all_rows, grad_values)
    grad_value, grad_out = reduce_grads(moves, part_value, part_out)
    return (slide_out[None], grad_value, grad_out)


def solution(mesh):
    placed = (
        P("group", "seq", None),
        P("group", "seq"),
        P(None, ("group", "seq")),
        P(None, ("group", "seq")),
        P(None, ("group", "seq")),
        P(),
        P(),
        P(),
        P(),
        P(),
        P("group", "seq", None),
    )
    return jax.shard_map(
        shards,
        mesh=mesh,
        in_specs=placed,
        out_specs=(P("group", "seq", None), P("seq", None), P("seq", None)),
        check_vma=False,
    )
```

```python
import math

import jax
import jax.numpy as jnp
from jax import lax
from jax.experimental import pallas as pl
from jax.experimental.pallas import tpu as pltpu
from jax.sharding import PartitionSpec as P

HEADS = 16
HEAD = 48
RATE = 16
BLOCK = 32

epsilon = 1e-06
BOTH = ("group", "seq")


def rms_rows(values):
    values = values.astype(jnp.float32)
    return values * lax.rsqrt(jnp.mean(values * values, axis=-1, keepdims=True) + epsilon)


def mm(left, right):
    return jnp.dot(left, right, preferred_element_type=jnp.float32)


def mm_nt(left, right):
    return lax.dot_general(
        left, right, (((1,), (1,)), ((), ())), preferred_element_type=jnp.float32
    )


def mm_tn(left, right):
    return lax.dot_general(
        left, right, (((0,), (0,)), ((), ())), preferred_element_type=jnp.float32
    )


def mm_tt(left, right):
    return lax.dot_general(
        left, right, (((0,), (1,)), ((), ())), preferred_element_type=jnp.float32
    )


def project_t(weight, rows):
    return mm_tt(weight, rows).astype(jnp.bfloat16)


HEADS_A_STEP = 4


def own_body(q_ref, k_ref, v_ref, bias_ref, e_ref, m_ref, l_ref, o_ref):
    bias = bias_ref[...]
    for h in range(HEADS_A_STEP):
        at = slice(h * HEAD, (h + 1) * HEAD)
        scores = mm_tn(k_ref[at], q_ref[at]) * (1.0 / math.sqrt(HEAD)) + bias
        top = jnp.max(scores, axis=0, keepdims=True)
        exponent = jnp.exp(scores - top)
        m_ref[h] = top
        l_ref[h] = jnp.sum(exponent, axis=0, keepdims=True)
        low = exponent.astype(jnp.bfloat16)
        e_ref[h] = low
        o_ref[at] = mm(v_ref[at], low)


def far_body(
    q_ref, k_ref, v_ref, bias_ref, g_ref, e_ref, m_ref, l_ref, o_ref, att_ref, own_ref, far_ref
):
    bias = bias_ref[...]
    for h in range(HEADS_A_STEP):
        at = slice(h * HEAD, (h + 1) * HEAD)
        scores = mm_tn(k_ref[at], q_ref[at]) * (1.0 / math.sqrt(HEAD)) + bias
        top = jnp.maximum(jnp.max(scores, axis=0, keepdims=True), m_ref[h])
        ratio = jnp.exp(m_ref[h] - top)
        exponent = jnp.exp(scores - top)
        norm = 1.0 / (l_ref[h] * ratio + jnp.sum(exponent, axis=0, keepdims=True))
        low = exponent.astype(jnp.bfloat16)
        att_ref[at] = ((o_ref[at] * ratio + mm(v_ref[at], low)) * norm).astype(jnp.bfloat16)
        grads = g_ref[at].astype(jnp.float32) * norm
        far_ref[at] = mm_nt(grads.astype(jnp.bfloat16), low).astype(jnp.bfloat16)
        own_ref[at] = mm_nt((grads * ratio).astype(jnp.bfloat16), e_ref[h]).astype(jnp.bfloat16)


def head_specs(*arrays):
    specs = []
    for array in arrays:
        if array.ndim == 3:
            specs.append(pl.BlockSpec((HEADS_A_STEP,) + array.shape[1:], lambda i: (i, 0, 0)))
        elif array.shape[1] == 1:
            specs.append(pl.BlockSpec(array.shape, lambda i: (0, 0)))
        else:
            specs.append(pl.BlockSpec((HEADS_A_STEP * HEAD, array.shape[1]), lambda i: (i, 0)))
    return specs


def attend_own(queries, keys, values, bias):
    rows = queries.shape[1]
    outs = [
        jax.ShapeDtypeStruct((HEADS, keys.shape[1], rows), jnp.bfloat16),
        jax.ShapeDtypeStruct((HEADS, 1, rows), jnp.float32),
        jax.ShapeDtypeStruct((HEADS, 1, rows), jnp.float32),
        jax.ShapeDtypeStruct(queries.shape, jnp.float32),
    ]
    args = (queries, keys, values, bias)
    return pl.pallas_call(
        own_body,
        grid=(HEADS // HEADS_A_STEP,),
        in_specs=head_specs(*args),
        out_specs=head_specs(*outs),
        out_shape=outs,
        cost_estimate=pl.CostEstimate(
            flops=40 * HEADS * rows * rows * HEAD,
            transcendentals=HEADS * rows * rows,
            bytes_accessed=2 * HEADS * rows * rows,
        ),
        name="attend_own",
    )(*args)


def attend_far(queries, keys, values, bias, grads, own):
    rows = queries.shape[1]
    outs = [
        jax.ShapeDtypeStruct(queries.shape, jnp.bfloat16),
        jax.ShapeDtypeStruct(queries.shape, jnp.bfloat16),
        jax.ShapeDtypeStruct(keys.shape, jnp.bfloat16),
    ]
    args = (queries, keys, values, bias, grads) + tuple(own)
    return pl.pallas_call(
        far_body,
        grid=(HEADS // HEADS_A_STEP,),
        in_specs=head_specs(*args),
        out_specs=head_specs(*outs),
        out_shape=outs,
        cost_estimate=pl.CostEstimate(
            flops=40 * HEADS * rows * rows * HEAD,
            transcendentals=HEADS * rows * rows,
            bytes_accessed=2 * HEADS * rows * rows,
        ),
        name="attend_far",
    )(*args)


class Moves:
    def __init__(self, groups, seqs):
        self.groups, self.seqs = groups, seqs
        self.rests = seqs // 4
        self.ring = (groups // 2) * self.rests

    def seq_xor(self, value, bit):
        return lax.ppermute(value, "seq", [(s, s ^ bit) for s in range(self.seqs)])

    def core(self, value):
        return self.seq_xor(value, 1)

    def x(self, value):
        return self.seq_xor(value, 2)

    def y(self, value):
        return lax.ppermute(value, "group", [(g, g ^ 1) for g in range(self.groups)])

    def rest_shift(self, value, step):
        pairs = []
        for s in range(self.seqs):
            target = ((s // 4 + step) % self.rests) * 4 + s % 4
            pairs.append((s, target))
        return lax.ppermute(value, "seq", pairs)

    def ring_next(self, value):
        pairs = []
        for g in range(self.groups):
            for s in range(self.seqs):
                place = ((g // 2) * self.rests + s // 4 + 1) % self.ring
                to_g = (place // self.rests) * 2 + g % 2
                to_s = (place % self.rests) * 4 + s % 4
                pairs.append((g * self.seqs + s, to_g * self.seqs + to_s))
        return lax.ppermute(value, BOTH, pairs)


def take(array, index, axis):
    return lax.dynamic_index_in_dim(array, index, axis, keepdims=False)


def ffn_term(rows, chunks, hidden):
    gate = jnp.concatenate([c[:hidden] for c in chunks], axis=0)
    upward = jnp.concatenate([c[hidden : 2 * hidden] for c in chunks], axis=0)
    down = jnp.concatenate([c[2 * hidden :] for c in chunks], axis=0)
    active = (jax.nn.silu(mm_nt(rows, gate)) * mm_nt(rows, upward)).astype(jnp.bfloat16)
    return mm(active, down)


def ffn_body(count, hidden, has_start, rows_ref, *refs):
    chunks, out_ref = refs[:count], refs[-1]
    rows = rows_ref[...]
    total = refs[count][...] if has_start else None
    for at in range(0, count, 2):
        pair = chunks[at : at + 2]
        proj = jnp.concatenate(
            [c[:hidden] for c in pair] + [c[hidden : 2 * hidden] for c in pair], axis=0
        )
        down = jnp.concatenate([c[2 * hidden :] for c in pair], axis=0)
        both = mm_nt(rows, proj)
        gate, upward = both[:, : 2 * hidden], both[:, 2 * hidden :]
        active = (gate / (1.0 + jnp.exp(-gate)) * upward).astype(jnp.bfloat16)
        term = mm(active, down)
        total = term if total is None else total + term
    out_ref[...] = total.astype(out_ref.dtype)


def ffn_kernel(rows, chunks, hidden, start, first, steps, block, dtype):
    width = rows.shape[1]
    row_spec = pl.BlockSpec((block, width), lambda i: (i + first, 0))
    whole = [pl.BlockSpec(c.shape, lambda i: (0, 0)) for c in chunks]
    return pl.pallas_call(
        lambda *refs: ffn_body(len(chunks), hidden, start is not None, *refs),
        grid=(steps,),
        in_specs=[row_spec] + whole + ([row_spec] if start is not None else []),
        out_specs=pl.BlockSpec((block, width), lambda i: (i, 0)),
        out_shape=jax.ShapeDtypeStruct((steps * block, width), dtype),
        cost_estimate=pl.CostEstimate(
            flops=6 * steps * block * width * hidden * len(chunks),
            transcendentals=steps * block * hidden * len(chunks),
            bytes_accessed=2 * width * (steps * block + 3 * hidden * len(chunks)),
        ),
        name="ffn_term",
    )(rows, *chunks, *([start] if start is not None else []))


def flip_blocks(rows):
    width = rows.shape[1]
    return rows.reshape(-1, BLOCK, width)[::-1].reshape(-1, width)


def encode(moves, tile_rows, row_count, w_gate, w_up, w_down_t, w_embed):
    hidden = w_gate.shape[1]
    half = tile_rows.shape[0] // 2
    spare = half - BLOCK
    chunk = jnp.concatenate([w_gate.T, w_up.T, w_down_t.T], axis=0)
    ringed = [chunk]
    for _ in range(moves.ring - 1):
        ringed.append(moves.ring_next(ringed[-1]))
    chunks = [[c, moves.core(c)] for c in ringed]
    extra = moves.y(flip_blocks(tile_rows[half : half + spare]))
    own_blocks = (row_count + BLOCK - 1) // BLOCK
    kept = (1 + jnp.arange(spare) // BLOCK) < own_blocks
    level = jnp.concatenate(
        [tile_rows[:BLOCK], jnp.where(kept[:, None], tile_rows[BLOCK:half], extra)], axis=0
    )
    normed = rms_rows(level).astype(jnp.bfloat16)
    part = half // 2
    first, second = normed[:part], normed[part:]
    first = jnp.concatenate([first, moves.x(first)], axis=0)
    second = jnp.concatenate([second, moves.y(second)], axis=0)
    rows = jnp.concatenate([moves.y(first), moves.x(second), first, second], axis=0)
    early = [c for pair in chunks[:-1] for c in pair]
    if hidden % 16 == 0 and early:
        begun = ffn_kernel(rows, early, hidden, None, 0, 2, 2 * half, jnp.float32)
        low = ffn_kernel(rows, chunks[-1], hidden, begun, 0, 2, half, jnp.bfloat16)
        mixed = ffn_kernel(rows, chunks[-1], hidden, begun, 2, 2, half, jnp.float32)
    else:
        mixed = ffn_term(rows, [c for pair in chunks for c in pair], hidden)
        low, mixed = mixed[: 2 * half].astype(jnp.bfloat16), mixed[2 * half :]
    first = mixed[:half] + moves.y(low[:half]).astype(jnp.float32)
    second = mixed[half:] + moves.x(low[half:]).astype(jnp.float32)
    first = first[:part] + moves.x(first[part:].astype(jnp.bfloat16)).astype(jnp.float32)
    second = second[:part] + moves.y(second[part:].astype(jnp.bfloat16)).astype(jnp.float32)
    mixed = jnp.concatenate([first, second], axis=0)
    embedded = rms_rows(level.astype(jnp.float32) + mixed).astype(jnp.bfloat16)
    slide_part = mm(embedded, w_embed).astype(jnp.bfloat16)
    back = moves.y(flip_blocks(slide_part[BLOCK:]))
    return jnp.concatenate([slide_part, back], axis=0)


def reduce_grads(moves, part_value, part_out):
    seqs = moves.seqs
    features, width = part_value.shape
    seq_index, group_index = lax.axis_index("seq"), lax.axis_index("group")
    core_bit, x_bit, rest = seq_index % 2, (seq_index // 2) % 2, seq_index // 4
    y_bit = group_index % 2
    share = features // seqs // 2
    low = jnp.bfloat16

    def halve(array, bit, axis, move):
        kept = take(array, bit, axis).astype(jnp.float32)
        return kept + move(take(array, 1 - bit, axis).astype(low)).astype(jnp.float32)

    def split(array):
        return array.reshape(moves.rests, 2, 2, 2, share, width)

    value = halve(split(part_value), core_bit, 2, moves.core)
    out = halve(split(part_out), core_bit, 2, moves.core)
    value = halve(value, x_bit, 1, moves.x)
    out = halve(out, y_bit, 2, moves.y)
    value = halve(value, y_bit, 1, moves.y)
    out = halve(out, x_bit, 1, moves.x)
    both = jnp.concatenate([value, out], axis=2)
    total = take(both, rest, 0)
    sent = both.astype(low)
    for step in range(1, moves.rests):
        block = take(sent, (rest + step) % moves.rests, 0)
        total = total + moves.rest_shift(block, step).astype(jnp.float32)
    total = total.astype(low)
    if moves.groups > 2:
        fellows = [list(range(bit, moves.groups, 2)) for bit in range(2)]
        everyone = lax.all_gather(total, "group", axis=0, axis_index_groups=fellows)
        total = jnp.sum(everyone.astype(jnp.float32), axis=0).astype(low)
    other = moves.y(total)
    top = jnp.where(y_bit == 0, total, other)
    bottom = jnp.where(y_bit == 0, other, total)
    full = jnp.concatenate([top, bottom], axis=0).astype(jnp.float32)
    return full[:, :width], full[:, width:]


def gather_far(moves, block):
    bit = moves.seqs // 2
    while bit >= 1:
        block = jnp.concatenate([block, moves.seq_xor(block, bit)], axis=0)
        bit //= 2
    return block


def shards(
    tiles, tile_counts, w_gate, w_up, w_down_t, w_embed, w_query, w_key, w_value, w_out, cotangent
):
    moves = Moves(lax.axis_size("group"), lax.axis_size("seq"))
    tile_rows = tiles[0]
    row_count = tile_counts[0, 0]
    seq_len = tile_rows.shape[0]
    live = seq_len - BLOCK
    is_valid = jnp.arange(live) < row_count
    grad_y = jnp.where(is_valid[:, None], cotangent[0, :live], jnp.zeros((), cotangent.dtype))
    grad_att = mm_nt(w_out, grad_y).astype(jnp.bfloat16)

    slide_tok = encode(moves, tile_rows, row_count, w_gate, w_up, w_down_t, w_embed)
    slide_normed = rms_rows(slide_tok).astype(jnp.bfloat16)
    width = slide_normed.shape[1]
    dilated = seq_len // RATE
    held = live // RATE
    far_count = ((row_count + RATE - 1) // RATE).astype(jnp.bfloat16)
    far_rows = gather_far(
        moves,
        jnp.concatenate(
            [
                slide_normed.reshape(held, RATE, width)[:, 0],
                jnp.full((dilated - held, width), far_count, jnp.bfloat16),
            ],
            axis=0,
        ),
    )
    far_blocks = far_rows.reshape(moves.seqs, dilated, width)
    far_valid = (
        jnp.arange(dilated)[None, :] < far_blocks[:, dilated - 1, :1].astype(jnp.float32)
    ).reshape(-1)
    bias_own = jnp.where(is_valid, 0.0, -1e30).astype(jnp.float32)[:, None]
    bias_far = jnp.where(far_valid, 0.0, -1e30).astype(jnp.float32)[:, None]
    queries = project_t(w_query, slide_normed)
    own = attend_own(
        queries, project_t(w_key, slide_normed), project_t(w_value, slide_normed), bias_own
    )
    attended, grads_own, grads_far = attend_far(
        queries, project_t(w_key, far_rows), project_t(w_value, far_rows), bias_far, grad_att, own
    )
    output = slide_tok.astype(jnp.float32) + mm_tn(attended, w_out)
    slide_out = jnp.where(is_valid[:, None], output, 0.0).astype(jnp.bfloat16)
    slide_out = jnp.concatenate([slide_out, jnp.zeros((BLOCK, width), jnp.bfloat16)], axis=0)
    part_out = mm(attended, grad_y)
    part_value = mm_tt(slide_normed, grads_own) + mm_tt(far_rows, grads_far)
    grad_value, grad_out = reduce_grads(moves, part_value, part_out)
    return (slide_out[None], grad_value, grad_out)


def solution(mesh):
    placed = (
        P("group", "seq", None),
        P("group", "seq"),
        P(None, ("group", "seq")),
        P(None, ("group", "seq")),
        P(None, ("group", "seq")),
        P(),
        P(),
        P(),
        P(),
        P(),
        P("group", "seq", None),
    )
    return jax.shard_map(
        shards,
        mesh=mesh,
        in_specs=placed,
        out_specs=(P("group", "seq", None), P("seq", None), P("seq", None)),
        check_vma=False,
    )
```

```python
import math

import jax
import jax.numpy as jnp
from jax import lax
from jax.experimental import pallas as pl
from jax.experimental.pallas import tpu as pltpu
from jax.sharding import PartitionSpec as P


HEADS = 16
HEAD = 48
RATE = 16
BLOCK = 32

epsilon = 1e-06
BOTH = ("group", "seq")


def rms_rows(values):
    values = values.astype(jnp.float32)
    return values * lax.rsqrt(jnp.mean(values * values, axis=-1, keepdims=True) + epsilon)


def mm(left, right):
    return jnp.dot(left, right, preferred_element_type=jnp.float32)


def mm_nt(left, right):
    return lax.dot_general(
        left, right, (((1,), (1,)), ((), ())), preferred_element_type=jnp.float32
    )


def mm_tn(left, right):
    return lax.dot_general(
        left, right, (((0,), (0,)), ((), ())), preferred_element_type=jnp.float32
    )


def mm_tt(left, right):
    return lax.dot_general(
        left, right, (((0,), (1,)), ((), ())), preferred_element_type=jnp.float32
    )


def project_t(weight, rows):
    return mm_tt(weight, rows).astype(jnp.bfloat16)


HEADS_A_CALL = 8


def own_body(rows_ref, wq_ref, wk_ref, wv_ref, bias_ref, q_ref, e_ref, m_ref, l_ref, o_ref):
    bias = bias_ref[...]
    rows = rows_ref[...]
    q_ref[...] = project_t(wq_ref[...], rows)
    keys, values = project_t(wk_ref[...], rows), project_t(wv_ref[...], rows)
    for h in range(HEADS_A_CALL):
        at = slice(h * HEAD, (h + 1) * HEAD)
        scores = mm_tn(keys[at], q_ref[at]) * (1.0 / math.sqrt(HEAD)) + bias
        top = jnp.max(scores, axis=0, keepdims=True)
        exponent = jnp.exp(scores - top)
        m_ref[h] = top
        l_ref[h] = jnp.sum(exponent, axis=0, keepdims=True)
        low = exponent.astype(jnp.bfloat16)
        e_ref[h] = low
        o_ref[at] = mm(values[at], low)


def far_body(
    rows_ref, wk_ref, wv_ref, bias_ref, g_ref, q_ref, e_ref, m_ref, l_ref, o_ref,
    att_ref, own_ref, far_ref,
):
    bias = bias_ref[...]
    rows = rows_ref[...]
    keys, values = project_t(wk_ref[...], rows), project_t(wv_ref[...], rows)
    for h in range(HEADS_A_CALL):
        at = slice(h * HEAD, (h + 1) * HEAD)
        scores = mm_tn(keys[at], q_ref[at]) * (1.0 / math.sqrt(HEAD)) + bias
        top = jnp.maximum(jnp.max(scores, axis=0, keepdims=True), m_ref[h])
        ratio = jnp.exp(m_ref[h] - top)
        exponent = jnp.exp(scores - top)
        norm = 1.0 / (l_ref[h] * ratio + jnp.sum(exponent, axis=0, keepdims=True))
        low = exponent.astype(jnp.bfloat16)
        att_ref[at] = ((o_ref[at] * ratio + mm(values[at], low)) * norm).astype(jnp.bfloat16)
        grads = g_ref[at].astype(jnp.float32) * norm
        far_ref[at] = mm_nt(grads.astype(jnp.bfloat16), low).astype(jnp.bfloat16)
        own_ref[at] = mm_nt((grads * ratio).astype(jnp.bfloat16), e_ref[h]).astype(jnp.bfloat16)


def whole_spec(array):
    return pl.BlockSpec(array.shape, lambda i: (0,) * array.ndim)


def weight_spec(array, part):
    return pl.BlockSpec((array.shape[0], HEADS_A_CALL * HEAD), lambda i: (0, part))


def feature_spec(array, part):
    return pl.BlockSpec((HEADS_A_CALL * HEAD, array.shape[1]), lambda i: (part, 0))


def attend_own(part, rows, w_query, w_key, w_value, bias):
    count = rows.shape[0]
    features = HEADS_A_CALL * HEAD
    outs = [
        jax.ShapeDtypeStruct((features, count), jnp.bfloat16),
        jax.ShapeDtypeStruct((HEADS_A_CALL, count, count), jnp.bfloat16),
        jax.ShapeDtypeStruct((HEADS_A_CALL, 1, count), jnp.float32),
        jax.ShapeDtypeStruct((HEADS_A_CALL, 1, count), jnp.float32),
        jax.ShapeDtypeStruct((features, count), jnp.float32),
    ]
    return pl.pallas_call(
        own_body,
        grid=(1,),
        in_specs=[whole_spec(rows)]
        + [weight_spec(w, part) for w in (w_query, w_key, w_value)]
        + [whole_spec(bias)],
        out_specs=[whole_spec(o) for o in outs],
        out_shape=outs,
        cost_estimate=pl.CostEstimate(
            flops=40 * features * count * count,
            transcendentals=HEADS_A_CALL * count * count,
            bytes_accessed=2 * HEADS_A_CALL * count * count,
        ),
        name="attend_own",
    )(rows, w_query, w_key, w_value, bias)


def attend_far(part, rows, w_key, w_value, bias, grads, own):
    count, features = grads.shape[1], HEADS_A_CALL * HEAD
    outs = [
        jax.ShapeDtypeStruct((features, count), jnp.bfloat16),
        jax.ShapeDtypeStruct((features, count), jnp.bfloat16),
        jax.ShapeDtypeStruct((features, rows.shape[0]), jnp.bfloat16),
    ]
    return pl.pallas_call(
        far_body,
        grid=(1,),
        in_specs=[whole_spec(rows), weight_spec(w_key, part), weight_spec(w_value, part)]
        + [whole_spec(bias), feature_spec(grads, part)]
        + [whole_spec(o) for o in own],
        out_specs=[whole_spec(o) for o in outs],
        out_shape=outs,
        cost_estimate=pl.CostEstimate(
            flops=40 * features * count * count,
            transcendentals=HEADS_A_CALL * count * count,
            bytes_accessed=2 * HEADS_A_CALL * count * count,
        ),
        name="attend_far",
    )(rows, w_key, w_value, bias, grads, *own)


class Moves:
    def __init__(self, groups, seqs):
        self.groups, self.seqs = groups, seqs
        self.rests = seqs // 4
        self.ring = (groups // 2) * self.rests

    def seq_xor(self, value, bit):
        return lax.ppermute(value, "seq", [(s, s ^ bit) for s in range(self.seqs)])

    def core(self, value):
        return self.seq_xor(value, 1)

    def x(self, value):
        return self.seq_xor(value, 2)

    def y(self, value):
        return lax.ppermute(value, "group", [(g, g ^ 1) for g in range(self.groups)])

    def rest_shift(self, value, step):
        pairs = []
        for s in range(self.seqs):
            target = ((s // 4 + step) % self.rests) * 4 + s % 4
            pairs.append((s, target))
        return lax.ppermute(value, "seq", pairs)

    def ring_next(self, value):
        pairs = []
        for g in range(self.groups):
            for s in range(self.seqs):
                place = ((g // 2) * self.rests + s // 4 + 1) % self.ring
                to_g = (place // self.rests) * 2 + g % 2
                to_s = (place % self.rests) * 4 + s % 4
                pairs.append((g * self.seqs + s, to_g * self.seqs + to_s))
        return lax.ppermute(value, BOTH, pairs)


def take(array, index, axis):
    return lax.dynamic_index_in_dim(array, index, axis, keepdims=False)


def ffn_term(rows, chunks, hidden):
    gate = jnp.concatenate([c[:hidden] for c in chunks], axis=0)
    upward = jnp.concatenate([c[hidden : 2 * hidden] for c in chunks], axis=0)
    down = jnp.concatenate([c[2 * hidden :] for c in chunks], axis=0)
    active = (jax.nn.silu(mm_nt(rows, gate)) * mm_nt(rows, upward)).astype(jnp.bfloat16)
    return mm(active, down)


def pack_body(gate_ref, up_ref, down_ref, out_ref):
    width, hidden = gate_ref.shape
    lanes = 2 * hidden
    out_ref[:width] = jnp.concatenate([gate_ref[...], up_ref[...]], axis=1)
    for tile in range(width // lanes):
        block = down_ref[tile * lanes : (tile + 1) * lanes].astype(jnp.float32)
        out_ref[width + tile * hidden : width + (tile + 1) * hidden] = block.T.astype(jnp.bfloat16)


def pack_weights(w_gate, w_up, w_down_t):
    width, hidden = w_gate.shape
    return pl.pallas_call(
        pack_body,
        out_shape=jax.ShapeDtypeStruct((width + width // 2, 2 * hidden), jnp.bfloat16),
        name="pack",
    )(w_gate, w_up, w_down_t)


def ffn_body(pieces, count, splits, *refs):
    rows_refs, chunk_refs = refs[:pieces], refs[pieces : pieces + count]
    at = pieces + count
    starts = refs[at:-splits] if len(refs) - splits > at else None
    outs = refs[-splits:]
    rows = jnp.concatenate([r[...] for r in rows_refs], axis=0)
    total = None if starts is None else jnp.concatenate([r[...] for r in starts], axis=0)
    width = rows.shape[1]
    lanes = chunk_refs[0].shape[1]
    hidden = lanes // 2
    is_low = lax.broadcasted_iota(jnp.int32, (rows.shape[0], lanes), 1) < hidden
    actives, downs = [], []
    for at in range(0, count, 2):
        pair = chunk_refs[at : at + 2]
        both = mm(rows, jnp.concatenate([c[:width] for c in pair], axis=1))
        even, odd = both[:, :lanes], both[:, lanes:]
        gate = jnp.where(is_low, even, pltpu.roll(odd, hidden, 1))
        upward = jnp.where(is_low, pltpu.roll(even, hidden, 1), odd)
        actives.append((gate / (1.0 + jnp.exp(-gate)) * upward).astype(jnp.bfloat16))
        for c in pair:
            tiles = [
                c[width + tile * hidden : width + (tile + 1) * hidden]
                for tile in range(width // lanes)
            ]
            downs.append(jnp.concatenate(tiles, axis=1))
    term = mm(jnp.concatenate(actives, axis=1), jnp.concatenate(downs, axis=0))
    total = term if total is None else total + term
    share = total.shape[0] // splits
    for i, out in enumerate(outs):
        out[...] = total[i * share : (i + 1) * share].astype(out.dtype)


def ffn_kernel(rows, chunks, starts, splits, dtype):
    width = rows[0].shape[1]
    height = sum(r.shape[0] for r in rows)
    units = len(chunks) * chunks[0].shape[1] // 2
    return pl.pallas_call(
        lambda *refs: ffn_body(len(rows), len(chunks), splits, *refs),
        out_shape=[jax.ShapeDtypeStruct((height // splits, width), dtype)] * splits,
        cost_estimate=pl.CostEstimate(
            flops=6 * height * width * units,
            transcendentals=height * units,
            bytes_accessed=2 * width * (height + 3 * units),
        ),
    )(*rows, *chunks, *(starts or []))


def flip_blocks(rows):
    width = rows.shape[1]
    return rows.reshape(-1, BLOCK, width)[::-1].reshape(-1, width)


def encode(moves, tile_rows, row_count, w_gate, w_up, w_down_t, w_embed):
    hidden = w_gate.shape[1]
    packed = 2 * hidden == 128 and moves.ring > 1
    half = tile_rows.shape[0] // 2
    part = half // 2
    spare = half - BLOCK
    low = jnp.bfloat16
    if packed:
        chunk = pack_weights(w_gate, w_up, w_down_t)
    else:
        chunk = jnp.concatenate([w_gate.T, w_up.T, w_down_t.T], axis=0)
    ringed = [chunk]
    for _ in range(1, moves.ring):
        ringed.append(moves.ring_next(ringed[-1]))
    chunks = []
    for c in ringed:
        chunks.append([c, moves.core(c)])
    extra = moves.y(flip_blocks(tile_rows[half : half + spare]))
    own_blocks = (row_count + BLOCK - 1) // BLOCK
    kept = (1 + jnp.arange(spare) // BLOCK) < own_blocks
    level = jnp.concatenate(
        [tile_rows[:BLOCK], jnp.where(kept[:, None], tile_rows[BLOCK:half], extra)], axis=0
    )
    normed = rms_rows(level).astype(low)
    first, second = normed[:part], normed[part:]
    first = jnp.concatenate([first, moves.x(first)], axis=0)
    second = jnp.concatenate([second, moves.y(second)], axis=0)
    first_y = moves.y(first)
    second_x = moves.x(second)
    early = [c for pair in chunks[:-1] for c in pair]
    if packed:
        begun = ffn_kernel([first_y, second_x, first, second], early, None, 8, jnp.float32)
        sent = ffn_kernel([first_y, second_x], chunks[-1], begun[:4], 4, low)
        kept = ffn_kernel([first, second], chunks[-1], begun[4:], 4, jnp.float32)
    else:
        rows = jnp.concatenate([first_y, second_x, first, second], axis=0)
        mixed = ffn_term(rows, [c for pair in chunks for c in pair], hidden)
        pieces = [mixed[i * part : (i + 1) * part] for i in range(8)]
        sent, kept = [p.astype(low) for p in pieces[:4]], pieces[4:]
    first_on = moves.y(sent[1])
    second_on = moves.x(sent[3])
    first_own = moves.y(sent[0])
    second_own = moves.x(sent[2])
    first_end = moves.x((kept[1] + first_on.astype(jnp.float32)).astype(low))
    second_end = moves.y((kept[3] + second_on.astype(jnp.float32)).astype(low))
    first = kept[0] + first_own.astype(jnp.float32) + first_end.astype(jnp.float32)
    second = kept[2] + second_own.astype(jnp.float32) + second_end.astype(jnp.float32)
    mixed = jnp.concatenate([first, second], axis=0)
    embedded = rms_rows(level.astype(jnp.float32) + mixed).astype(low)
    slide_part = mm(embedded, w_embed).astype(low)
    normed_part = rms_rows(slide_part).astype(low)
    far_back = moves.y(flip_blocks(normed_part[BLOCK:])[::RATE])
    back = moves.y(flip_blocks(slide_part[BLOCK:]))
    far = jnp.concatenate([normed_part[::RATE], far_back], axis=0)
    return jnp.concatenate([slide_part, back], axis=0), far


def reduce_grads(moves, part_value, part_out):
    seqs = moves.seqs
    features, width = part_value.shape
    seq_index, group_index = lax.axis_index("seq"), lax.axis_index("group")
    core_bit, x_bit, rest = seq_index % 2, (seq_index // 2) % 2, seq_index // 4
    y_bit = group_index % 2
    share = features // seqs // 2
    low = jnp.bfloat16

    def halve(array, bit, axis, move):
        kept = take(array, bit, axis).astype(jnp.float32)
        return kept + move(take(array, 1 - bit, axis).astype(low)).astype(jnp.float32)

    def split(array):
        return array.reshape(moves.rests, 2, 2, 2, share, width)

    value = halve(split(part_value), core_bit, 2, moves.core)
    out = halve(split(part_out), core_bit, 2, moves.core)
    value = halve(value, x_bit, 1, moves.x)
    out = halve(out, y_bit, 2, moves.y)
    value = halve(value, y_bit, 1, moves.y)
    out = halve(out, x_bit, 1, moves.x)
    both = jnp.concatenate([value, out], axis=2)
    total = take(both, rest, 0)
    sent = both.astype(low)
    for step in range(1, moves.rests):
        block = take(sent, (rest + step) % moves.rests, 0)
        total = total + moves.rest_shift(block, step).astype(jnp.float32)
    total = total.astype(low)
    if moves.groups > 2:
        fellows = [list(range(bit, moves.groups, 2)) for bit in range(2)]
        everyone = lax.all_gather(total, "group", axis=0, axis_index_groups=fellows)
        total = jnp.sum(everyone.astype(jnp.float32), axis=0).astype(low)
    other = moves.y(total)
    top = jnp.where(y_bit == 0, total, other)
    bottom = jnp.where(y_bit == 0, other, total)
    full = jnp.concatenate([top, bottom], axis=0).astype(jnp.float32)
    return full[:, :width], full[:, width:]


def gather_far(moves, block):
    bit = moves.seqs // 2
    while bit >= 1:
        block = jnp.concatenate([block, moves.seq_xor(block, bit)], axis=0)
        bit //= 2
    return block


def shards(
    tiles, tile_counts, w_gate, w_up, w_down_t, w_embed, w_query, w_key, w_value, w_out, cotangent
):
    moves = Moves(lax.axis_size("group"), lax.axis_size("seq"))
    tile_rows = tiles[0]
    row_count = tile_counts[0, 0]
    seq_len = tile_rows.shape[0]
    live = seq_len - BLOCK
    is_valid = jnp.arange(live) < row_count
    grad_y = jnp.where(is_valid[:, None], cotangent[0, :live], jnp.zeros((), cotangent.dtype))
    grad_att = mm_nt(w_out, grad_y).astype(jnp.bfloat16)

    slide_tok, own_far = encode(
        moves, tile_rows, row_count, w_gate, w_up, w_down_t, w_embed
    )
    slide_normed = rms_rows(slide_tok).astype(jnp.bfloat16)
    width = slide_normed.shape[1]
    dilated = seq_len // RATE
    held = live // RATE
    far_count = ((row_count + RATE - 1) // RATE).astype(jnp.bfloat16)
    far_rows = gather_far(
        moves,
        jnp.concatenate(
            [own_far, jnp.full((dilated - held, width), far_count, jnp.bfloat16)], axis=0
        ),
    )
    far_blocks = far_rows.reshape(moves.seqs, dilated, width)
    far_valid = (
        jnp.arange(dilated)[None, :] < far_blocks[:, dilated - 1, :1].astype(jnp.float32)
    ).reshape(-1)
    bias_own = jnp.where(is_valid, 0.0, -1e30).astype(jnp.float32)[:, None]
    bias_far = jnp.where(far_valid, 0.0, -1e30).astype(jnp.float32)[:, None]
    parts = range(HEADS // HEADS_A_CALL)
    own = []
    for part in parts:
        own.append(attend_own(part, slide_normed, w_query, w_key, w_value, bias_own))
    ends = [
        attend_far(part, far_rows, w_key, w_value, bias_far, grad_att, own[part])
        for part in parts
    ]
    attended, grads_own, grads_far = [
        jnp.concatenate(pieces, axis=0) for pieces in zip(*ends)
    ]
    output = slide_tok.astype(jnp.float32) + mm_tn(attended, w_out)
    slide_out = jnp.where(is_valid[:, None], output, 0.0).astype(jnp.bfloat16)
    slide_out = jnp.concatenate([slide_out, jnp.zeros((BLOCK, width), jnp.bfloat16)], axis=0)
    part_out = mm(attended, grad_y)
    part_value = mm_tt(slide_normed, grads_own) + mm_tt(far_rows, grads_far)
    grad_value, grad_out = reduce_grads(moves, part_value, part_out)
    return (slide_out[None], grad_value, grad_out)


def solution(mesh):
    placed = (
        P("group", "seq", None),
        P("group", "seq"),
        P(None, ("group", "seq")),
        P(None, ("group", "seq")),
        P(None, ("group", "seq")),
        P(),
        P(),
        P(),
        P(),
        P(),
        P("group", "seq", None),
    )

    return jax.shard_map(
        shards,
        mesh=mesh,
        in_specs=placed,
        out_specs=(P("group", "seq", None), P("seq", None), P("seq", None)),
        check_vma=False,
    )
```

```python
import math

import jax
import jax.numpy as jnp
from jax import lax
from jax.experimental import pallas as pl
from jax.experimental.pallas import tpu as pltpu
from jax.sharding import PartitionSpec as P


HEADS = 16
HEAD = 48
RATE = 16
BLOCK = 32

epsilon = 1e-06
BOTH = ("group", "seq")


def rms_rows(values):
    values = values.astype(jnp.float32)
    return values * lax.rsqrt(jnp.mean(values * values, axis=-1, keepdims=True) + epsilon)


def mm(left, right):
    return jnp.dot(left, right, preferred_element_type=jnp.float32)


def mm_nt(left, right):
    return lax.dot_general(
        left, right, (((1,), (1,)), ((), ())), preferred_element_type=jnp.float32
    )


def mm_tn(left, right):
    return lax.dot_general(
        left, right, (((0,), (0,)), ((), ())), preferred_element_type=jnp.float32
    )


def mm_tt(left, right):
    return lax.dot_general(
        left, right, (((0,), (1,)), ((), ())), preferred_element_type=jnp.float32
    )


def project_t(weight, rows):
    return mm_tt(weight, rows).astype(jnp.bfloat16)


HEADS_A_CALL = 8
HEADS_A_STEP = 4


def valid_column(count_ref, height):
    return lax.broadcasted_iota(jnp.int32, (height, 1), 0) < count_ref[0, 0]


def grads_in_body(count_ref, cotangent_ref, w_out_ref, grad_y_ref, grad_att_ref):
    height = grad_y_ref.shape[0]
    grad_y = cotangent_ref[:height].astype(jnp.float32)
    grad_y = jnp.where(valid_column(count_ref, height), grad_y, 0.0).astype(jnp.bfloat16)
    grad_y_ref[...] = grad_y
    grad_att_ref[...] = mm_nt(w_out_ref[...], grad_y).astype(jnp.bfloat16)


def grads_in(counts, cotangent, w_out, live):
    width = w_out.shape[0]
    return pl.pallas_call(
        grads_in_body,
        in_specs=[pl.BlockSpec(memory_space=pltpu.SMEM), NEAR, NEAR],
        out_specs=[NEAR] * 2,
        out_shape=[
            pltpu.VMEM((live, width), jnp.bfloat16),
            pltpu.VMEM((width, live), jnp.bfloat16),
        ],
        compiler_params=room(8),
        name="grads_in",
    )(counts, *near(cotangent, w_out))


FAR_AWAY = pl.BlockSpec(memory_space=pltpu.HBM)


def fetch(sources, targets, sems, first=0):
    copies = []
    for i, (source, target) in enumerate(zip(sources, targets)):
        copies.append(pltpu.make_async_copy(source, target, sems.at[first + i]))
        copies[-1].start()
    return copies


def own_body(
    part, count_ref, rows_in, wq_in, wk_in, wv_in, q_out, e_out, m_out, l_out, o_out,
    rows_ref, wq_ref, wk_ref, wv_ref, q_ref, e_ref, m_ref, l_ref, o_ref, sems,
):
    cut = pl.ds(part * HEADS_A_CALL * HEAD, HEADS_A_CALL * HEAD)
    got = fetch(
        (rows_in, wq_in.at[:, cut], wk_in.at[:, cut], wv_in.at[:, cut]),
        (rows_ref, wq_ref, wk_ref, wv_ref),
        sems,
    )
    got[0].wait()
    rows = rows_ref[...]
    bias = jnp.where(valid_column(count_ref, rows.shape[0]), 0.0, -1e30)
    got[1].wait()
    q_ref[...] = project_t(wq_ref[...], rows)
    got[2].wait()
    keys = project_t(wk_ref[...], rows)
    got[3].wait()
    values = project_t(wv_ref[...], rows)
    sent = fetch([q_ref], [q_out], sems, 4)
    for h in range(HEADS_A_CALL):
        at = slice(h * HEAD, (h + 1) * HEAD)
        scores = mm_tn(keys[at], q_ref[at]) * (1.0 / math.sqrt(HEAD)) + bias
        top = jnp.max(scores, axis=0, keepdims=True)
        exponent = jnp.exp(scores - top)
        m_ref[h] = top
        l_ref[h] = jnp.sum(exponent, axis=0, keepdims=True)
        low = exponent.astype(jnp.bfloat16)
        e_ref[h] = low
        sent += fetch([e_ref.at[h]], [e_out.at[h]], sems, 8 + h)
        o_ref[at] = mm(values[at], low)
    sent += fetch((m_ref, l_ref, o_ref), (m_out, l_out, o_out), sems, 5)
    for copy in sent:
        copy.wait()


def far_body(dilated, *refs):
    parts = HEADS // HEADS_A_CALL
    count = 6 + 5 * parts
    core_ref, ins, outs = refs[0], refs[1 : 1 + count], refs[1 + count : 6 + count]
    held, sems = refs[6 + count : 6 + 2 * count], refs[-1]
    keys_ref, values_ref, own_ref, far_ref, sum_ref = refs[-6:-1]
    got = fetch(ins, held, sems)
    rows_ref, wk_ref, wv_ref, g_ref = held[:4]
    grad_y_ref, normed_ref = held[-2:]
    att_ref = outs[0]
    got[0].wait()
    rows = rows_ref[...]
    place = lax.broadcasted_iota(jnp.int32, (dilated, 1), 0).astype(jnp.float32)
    pieces = []
    for end in range(dilated, rows.shape[0] + 1, dilated):
        pieces.append(jnp.where(place < rows_ref[end - 1 : end, :1].astype(jnp.float32), 0.0, -1e30))
    bias = jnp.concatenate(pieces, axis=0)
    got[1].wait()
    keys_ref[...] = project_t(wk_ref[...], rows)
    got[2].wait()
    values_ref[...] = project_t(wv_ref[...], rows)
    got[3].wait()

    for part in range(parts):
        for copy in got[4 + part * 5 : 9 + part * 5]:
            copy.wait()
        q_ref, e_ref, m_ref, l_ref, o_ref = held[4 + part * 5 : 9 + part * 5]
        first = part * HEADS_A_CALL * HEAD

        def step(i, _):
            for k in range(HEADS_A_STEP):
                h = i * HEADS_A_STEP + k
                here = pl.ds(pl.multiple_of(h * HEAD, HEAD), HEAD)
                at = pl.ds(pl.multiple_of(first + h * HEAD, HEAD), HEAD)
                scores = mm_tn(keys_ref[at], q_ref[here]) * (1.0 / math.sqrt(HEAD)) + bias
                top = jnp.maximum(jnp.max(scores, axis=0, keepdims=True), m_ref[h])
                ratio = jnp.exp(m_ref[h] - top)
                exponent = jnp.exp(scores - top)
                norm = 1.0 / (l_ref[h] * ratio + jnp.sum(exponent, axis=0, keepdims=True))
                low = exponent.astype(jnp.bfloat16)
                total = (o_ref[here] * ratio + mm(values_ref[at], low)) * norm
                att_ref[at] = total.astype(jnp.bfloat16)
                grads = g_ref[at].astype(jnp.float32) * norm
                far_ref[at] = mm_nt(grads.astype(jnp.bfloat16), low).astype(jnp.bfloat16)
                grads = (grads * ratio).astype(jnp.bfloat16)
                own_ref[at] = mm_nt(grads, e_ref[h]).astype(jnp.bfloat16)
            return 0

        lax.fori_loop(0, HEADS_A_CALL // HEADS_A_STEP, step, 0)

    def share_out(total, kept_ref, sent_ref):
        sum_ref[...] = total
        share = rows.shape[0] // dilated
        share = sum_ref.shape[0] // share
        for ref, bit in ((kept_ref, core_ref[0]), (sent_ref, 1 - core_ref[0])):
            pieces = []
            for first in range(0, sum_ref.shape[0], 2 * share):
                start = pl.multiple_of(first + bit * share, 8)
                pieces.append(sum_ref[pl.ds(start, share)])
            ref[...] = jnp.concatenate(pieces, axis=0).astype(ref.dtype)

    got[-2].wait()
    share_out(mm(att_ref[...], grad_y_ref[...]), outs[1], outs[2])
    got[-1].wait()
    total = mm_tt(normed_ref[...], own_ref[...]) + mm_tt(rows, far_ref[...])
    share_out(total, outs[3], outs[4])


def attend_own(part, counts, rows, w_query, w_key, w_value):
    count = rows.shape[0]
    features = HEADS_A_CALL * HEAD
    outs = [
        pltpu.HBM((features, count), jnp.bfloat16),
        pltpu.HBM((HEADS_A_CALL, count, count), jnp.bfloat16),
        pltpu.HBM((HEADS_A_CALL, 1, count), jnp.float32),
        pltpu.HBM((HEADS_A_CALL, 1, count), jnp.float32),
        pltpu.HBM((features, count), jnp.float32),
    ]
    cut = pltpu.VMEM((rows.shape[1], features), jnp.bfloat16)
    return pl.pallas_call(
        lambda *refs: own_body(part, *refs),
        in_specs=[pl.BlockSpec(memory_space=pltpu.SMEM)] + [FAR_AWAY] * 4,
        out_specs=[FAR_AWAY] * 5,
        out_shape=outs,
        scratch_shapes=[
            pltpu.VMEM(rows.shape, jnp.bfloat16),
            cut,
            cut,
            cut,
        ]
        + [pltpu.VMEM(o.shape, o.dtype) for o in outs]
        + [pltpu.SemaphoreType.DMA((8 + HEADS_A_CALL,))],
        compiler_params=room(24),
        cost_estimate=pl.CostEstimate(
            flops=40 * features * count * count,
            transcendentals=HEADS_A_CALL * count * count,
            bytes_accessed=2 * HEADS_A_CALL * count * count,
        ),
        name="attend_own",
    )(counts, *away(rows, w_query, w_key, w_value))


def attend_far(dilated, core_bit, rows, w_key, w_value, grads, own, grad_y, normed):
    width, count = grads.shape
    args = [rows, w_key, w_value, grads]
    args += [array for arrays in own for array in arrays] + [grad_y, normed]
    low = jnp.bfloat16
    cut = [pltpu.VMEM((width // 2, width), jnp.float32), pltpu.VMEM((width // 2, width), low)]
    return pl.pallas_call(
        lambda *refs: far_body(dilated, *refs),
        in_specs=[pl.BlockSpec(memory_space=pltpu.SMEM)] + [FAR_AWAY] * len(args),
        out_specs=[NEAR] * 5,
        out_shape=[pltpu.VMEM((width, count), low)] + cut + cut,
        scratch_shapes=[pltpu.VMEM(a.shape, a.dtype) for a in args]
        + [pltpu.VMEM((width, rows.shape[0]), low)] * 2
        + [
            pltpu.VMEM((width, count), low),
            pltpu.VMEM((width, rows.shape[0]), low),
            pltpu.VMEM((width, width), jnp.float32),
        ]
        + [pltpu.SemaphoreType.DMA((len(args),))],
        compiler_params=room(40),
        cost_estimate=pl.CostEstimate(
            flops=40 * width * count * count,
            transcendentals=HEADS * count * count,
            bytes_accessed=2 * HEADS * count * count,
        ),
        name="attend_far",
    )(core_bit, *away(*args))


def near(*arrays):
    return tuple(pltpu.with_memory_space_constraint(a, pltpu.VMEM) for a in arrays)


def room(mebibytes):
    return pltpu.CompilerParams(vmem_limit_bytes=mebibytes << 20)


def away(*arrays):
    return tuple(pltpu.with_memory_space_constraint(a, pltpu.HBM) for a in arrays)


NEAR = pl.BlockSpec(memory_space=pltpu.VMEM)


class Moves:
    def __init__(self, groups, seqs):
        self.groups, self.seqs = groups, seqs
        self.rests = seqs // 4
        self.ring = (groups // 2) * self.rests

    def seq_xor(self, value, bit):
        return lax.ppermute(value, "seq", [(s, s ^ bit) for s in range(self.seqs)])

    def core(self, value):
        return self.seq_xor(value, 1)

    def x(self, value):
        return self.seq_xor(value, 2)

    def y(self, value):
        return lax.ppermute(value, "group", [(g, g ^ 1) for g in range(self.groups)])

    def rest_shift(self, value, step):
        pairs = []
        for s in range(self.seqs):
            target = ((s // 4 + step) % self.rests) * 4 + s % 4
            pairs.append((s, target))
        return lax.ppermute(value, "seq", pairs)

    def ring_next(self, value):
        pairs = []
        for g in range(self.groups):
            for s in range(self.seqs):
                place = ((g // 2) * self.rests + s // 4 + 1) % self.ring
                to_g = (place // self.rests) * 2 + g % 2
                to_s = (place % self.rests) * 4 + s % 4
                pairs.append((g * self.seqs + s, to_g * self.seqs + to_s))
        return lax.ppermute(value, BOTH, pairs)


def take(array, index, axis):
    return lax.dynamic_index_in_dim(array, index, axis, keepdims=False)


def ffn_term(rows, chunks, hidden):
    gate = jnp.concatenate([c[:hidden] for c in chunks], axis=0)
    upward = jnp.concatenate([c[hidden : 2 * hidden] for c in chunks], axis=0)
    down = jnp.concatenate([c[2 * hidden :] for c in chunks], axis=0)
    active = (jax.nn.silu(mm_nt(rows, gate)) * mm_nt(rows, upward)).astype(jnp.bfloat16)
    return mm(active, down)


def pack_body(gate_ref, up_ref, down_ref, out_ref):
    hidden, width = gate_ref.shape
    lanes = 2 * hidden
    for tile in range(width // lanes):
        at = slice(tile * lanes, (tile + 1) * lanes)
        block = jnp.concatenate([gate_ref[:, at], up_ref[:, at]], axis=0)
        out_ref[at] = block.T
        out_ref[width + tile * hidden : width + (tile + 1) * hidden] = down_ref[:, at]


def pack_weights(w_gate, w_up, w_down_t):
    width, hidden = w_gate.shape
    return pl.pallas_call(
        pack_body,
        in_specs=[NEAR] * 3,
        out_specs=NEAR,
        out_shape=pltpu.VMEM((width + width // 2, 2 * hidden), jnp.bfloat16),
        compiler_params=room(4),
        name="pack",
    )(*near(w_gate.T, w_up.T, w_down_t.T))


def ffn_body(pieces, count, splits, *refs):
    rows_refs, chunk_refs = refs[:pieces], refs[pieces : pieces + count]
    at = pieces + count
    starts = refs[at:-splits] if len(refs) - splits > at else None
    outs = refs[-splits:]
    rows = jnp.concatenate([r[...] for r in rows_refs], axis=0)
    total = None if starts is None else jnp.concatenate([r[...] for r in starts], axis=0)
    width = rows.shape[1]
    lanes = chunk_refs[0].shape[1]
    hidden = lanes // 2
    is_low = lax.broadcasted_iota(jnp.int32, (rows.shape[0], lanes), 1) < hidden
    actives, downs = [], []
    for at in range(0, count, 2):
        pair = chunk_refs[at : at + 2]
        both = mm(rows, jnp.concatenate([c[:width] for c in pair], axis=1))
        even, odd = both[:, :lanes], both[:, lanes:]
        gate = jnp.where(is_low, even, pltpu.roll(odd, hidden, 1))
        upward = jnp.where(is_low, pltpu.roll(even, hidden, 1), odd)
        actives.append((gate / (1.0 + jnp.exp(-gate)) * upward).astype(jnp.bfloat16))
        for c in pair:
            tiles = [
                c[width + tile * hidden : width + (tile + 1) * hidden]
                for tile in range(width // lanes)
            ]
            downs.append(jnp.concatenate(tiles, axis=1))
    term = mm(jnp.concatenate(actives, axis=1), jnp.concatenate(downs, axis=0))
    total = term if total is None else total + term
    share = total.shape[0] // splits
    for i, out in enumerate(outs):
        out[...] = total[i * share : (i + 1) * share].astype(out.dtype)


def ffn_kernel(rows, chunks, starts, splits, dtype):
    width = rows[0].shape[1]
    height = sum(r.shape[0] for r in rows)
    units = len(chunks) * chunks[0].shape[1] // 2
    return pl.pallas_call(
        lambda *refs: ffn_body(len(rows), len(chunks), splits, *refs),
        in_specs=[NEAR] * (len(rows) + len(chunks) + len(starts or [])),
        out_specs=[NEAR] * splits,
        out_shape=[pltpu.VMEM((height // splits, width), dtype)] * splits,
        cost_estimate=pl.CostEstimate(
            flops=6 * height * width * units,
            transcendentals=height * units,
            bytes_accessed=2 * width * (height + 3 * units),
        ),
        compiler_params=room(24),
    )(*near(*rows, *chunks, *(starts or [])))


def norm_rows(values):
    return values * lax.rsqrt(jnp.mean(values * values, axis=-1, keepdims=True) + epsilon)


def join_body(first_ref, second_ref, out_ref):
    height = first_ref.shape[0]
    out_ref[:height] = first_ref[...]
    out_ref[height:] = second_ref[...]


def join(first, second):
    height, width = first.shape
    return pl.pallas_call(
        join_body,
        in_specs=[NEAR] * 2,
        out_specs=NEAR,
        out_shape=pltpu.VMEM((2 * height, width), first.dtype),
        compiler_params=room(2),
        name="join",
    )(*near(first, second))


def picked(rows, sources):
    at = lax.broadcasted_iota(jnp.int32, (sources.shape[0], rows.shape[0]), 1)
    return mm((at == sources).astype(jnp.bfloat16), rows)


def finish_body(count_ref, level_ref, *refs):
    sums, w_embed_ref = refs[:6], refs[6]
    slide_ref, back_ref, far_ref, far_send_ref = refs[7:]
    low = jnp.bfloat16
    mixed = []
    for kept, own, end in (sums[:3], sums[3:]):
        mixed.append(kept[...] + own[...].astype(jnp.float32) + end[...].astype(jnp.float32))
    encoded = level_ref[...].astype(jnp.float32) + jnp.concatenate(mixed, axis=0)
    slide = mm(norm_rows(encoded).astype(low), w_embed_ref[...]).astype(low)
    slide_ref[...] = slide
    half, blocks = slide.shape[0], back_ref.shape[0] // BLOCK
    for block in range(blocks):
        source = (blocks - block) * BLOCK
        back_ref[block * BLOCK : (block + 1) * BLOCK] = slide[source : source + BLOCK]
    normed = norm_rows(slide.astype(jnp.float32)).astype(low)
    place = lax.broadcasted_iota(jnp.int32, (far_ref.shape[0], 1), 0)
    own_far, sent_far = half // RATE, blocks * BLOCK // RATE
    far = picked(normed, jnp.where(place < own_far, place * RATE, -1))
    far_count = ((count_ref[0, 0] + RATE - 1) // RATE).astype(jnp.float32)
    far_ref[...] = jnp.where(place < own_far + sent_far, far, far_count).astype(low)
    step = (place - own_far) * RATE
    source = (blocks - step // BLOCK) * BLOCK + step % BLOCK
    is_sent = (place >= own_far) & (place < own_far + sent_far)
    far_send_ref[...] = picked(normed, jnp.where(is_sent, source, -1)).astype(low)


def finish(counts, level, sums, w_embed, dilated):
    half, width = level.shape[0], w_embed.shape[1]
    low = jnp.bfloat16
    return pl.pallas_call(
        finish_body,
        in_specs=[pl.BlockSpec(memory_space=pltpu.SMEM)] + [NEAR] * 8,
        out_specs=[NEAR] * 4,
        out_shape=[
            pltpu.VMEM((half, width), low),
            pltpu.VMEM((half - BLOCK, width), low),
            pltpu.VMEM((dilated, width), low),
            pltpu.VMEM((dilated, width), low),
        ],
        compiler_params=room(12),
        name="finish",
    )(counts, *near(level, *sums, w_embed))


def tokens_body(part_ref, back_ref, slide_ref, normed_ref):
    slide = jnp.concatenate([part_ref[...], back_ref[...]], axis=0)
    slide_ref[...] = slide
    normed_ref[...] = norm_rows(slide.astype(jnp.float32)).astype(jnp.bfloat16)


def tokens(part, back):
    shape = (part.shape[0] + back.shape[0], part.shape[1])
    return pl.pallas_call(
        tokens_body,
        in_specs=[NEAR] * 2,
        out_specs=[NEAR] * 2,
        out_shape=[pltpu.HBM(shape, jnp.bfloat16)] * 2,
        compiler_params=room(6),
        name="tokens",
    )(*near(part, back))


def flip_blocks(rows):
    width = rows.shape[1]
    return rows.reshape(-1, BLOCK, width)[::-1].reshape(-1, width)


def encode(moves, counts, tile_rows, row_count, w_gate, w_up, w_down_t, w_embed):
    hidden = w_gate.shape[1]
    packed = 2 * hidden == 128 and moves.ring > 1
    half = tile_rows.shape[0] // 2
    part = half // 2
    spare = half - BLOCK
    low = jnp.bfloat16
    if packed:
        chunk = pack_weights(w_gate, w_up, w_down_t)
    else:
        chunk = jnp.concatenate([w_gate.T, w_up.T, w_down_t.T], axis=0)
    ringed = [chunk]
    for _ in range(1, moves.ring):
        ringed.append(moves.ring_next(ringed[-1]))
    chunks = []
    for c in ringed:
        chunks.append([c, moves.core(c)])
    extra = moves.y(flip_blocks(tile_rows[half : half + spare]))
    own_blocks = (row_count + BLOCK - 1) // BLOCK
    kept = (1 + jnp.arange(spare) // BLOCK) < own_blocks
    level = jnp.concatenate(
        [tile_rows[:BLOCK], jnp.where(kept[:, None], tile_rows[BLOCK:half], extra)], axis=0
    )
    normed = rms_rows(level).astype(low)
    first, second = normed[:part], normed[part:]
    first = jnp.concatenate([first, moves.x(first)], axis=0)
    second = jnp.concatenate([second, moves.y(second)], axis=0)
    first_y = moves.y(first)
    second_x = moves.x(second)
    early = [c for pair in chunks[:-1] for c in pair]
    if packed:
        begun = ffn_kernel([first_y, second_x, first, second], early, None, 8, jnp.float32)
        sent = ffn_kernel([first_y, second_x], chunks[-1], begun[:4], 4, low)
        kept = ffn_kernel([first, second], chunks[-1], begun[4:], 4, jnp.float32)
    else:
        rows = jnp.concatenate([first_y, second_x, first, second], axis=0)
        mixed = ffn_term(rows, [c for pair in chunks for c in pair], hidden)
        pieces = [mixed[i * part : (i + 1) * part] for i in range(8)]
        sent, kept = [p.astype(low) for p in pieces[:4]], pieces[4:]
    first_on = moves.y(sent[1])
    second_on = moves.x(sent[3])
    first_own = moves.y(sent[0])
    second_own = moves.x(sent[2])
    first_end = moves.x((kept[1] + first_on.astype(jnp.float32)).astype(low))
    second_end = moves.y((kept[3] + second_on.astype(jnp.float32)).astype(low))
    dilated = tile_rows.shape[0] // RATE
    sums = (kept[0], first_own, first_end, kept[2], second_own, second_end)
    slide_part, to_back, far_own, far_send = finish(counts, level, sums, w_embed, dilated)
    far_got = moves.y(far_send)
    back = moves.y(to_back)
    place = jnp.arange(dilated)[:, None]
    is_got = (place >= half // RATE) & (place < (half + spare) // RATE)
    return tokens(slide_part, back), jnp.where(is_got, far_got, far_own)


def reduce_grads(moves, out_kept, out_sent, value_kept, value_sent):
    seqs = moves.seqs
    features, width = 2 * out_kept.shape[0], out_kept.shape[1]
    seq_index, group_index = lax.axis_index("seq"), lax.axis_index("group")
    x_bit, rest = (seq_index // 2) % 2, seq_index // 4
    y_bit = group_index % 2
    share = features // seqs // 2
    low = jnp.bfloat16

    def halve(array, bit, axis, move):
        kept = take(array, bit, axis).astype(jnp.float32)
        return kept + move(take(array, 1 - bit, axis).astype(low)).astype(jnp.float32)

    def with_core(kept, sent):
        total = kept + moves.core(sent).astype(jnp.float32)
        return total.reshape(moves.rests, 2, 2, share, width)

    out = with_core(out_kept, out_sent)
    value = with_core(value_kept, value_sent)
    value = halve(value, x_bit, 1, moves.x)
    out = halve(out, y_bit, 2, moves.y)
    value = halve(value, y_bit, 1, moves.y)
    out = halve(out, x_bit, 1, moves.x)
    both = jnp.concatenate([value, out], axis=2)
    total = take(both, rest, 0)
    sent = both.astype(low)
    for step in range(1, moves.rests):
        block = take(sent, (rest + step) % moves.rests, 0)
        total = total + moves.rest_shift(block, step).astype(jnp.float32)
    total = total.astype(low)
    if moves.groups > 2:
        fellows = [list(range(bit, moves.groups, 2)) for bit in range(2)]
        everyone = lax.all_gather(total, "group", axis=0, axis_index_groups=fellows)
        total = jnp.sum(everyone.astype(jnp.float32), axis=0).astype(low)
    other = moves.y(total)
    top = jnp.where(y_bit == 0, total, other)
    bottom = jnp.where(y_bit == 0, other, total)
    full = jnp.concatenate([top, bottom], axis=0).astype(jnp.float32)
    return full[:, :width], full[:, width:]


def gather_far(moves, block):
    bit = moves.seqs // 2
    while bit >= 1:
        block = join(block, moves.seq_xor(block, bit))
        bit //= 2
    return block


def shards(
    tiles, tile_counts, w_gate, w_up, w_down_t, w_embed, w_query, w_key, w_value, w_out, cotangent
):
    moves = Moves(lax.axis_size("group"), lax.axis_size("seq"))
    tile_rows = tiles[0]
    row_count = tile_counts[0, 0]
    seq_len = tile_rows.shape[0]
    live = seq_len - BLOCK
    is_valid = jnp.arange(live) < row_count
    grad_y, grad_att = grads_in(tile_counts, cotangent[0], w_out, live)
    (slide_tok, slide_normed), far_block = encode(
        moves, tile_counts, tile_rows, row_count, w_gate, w_up, w_down_t, w_embed
    )
    width = slide_tok.shape[1]
    dilated = seq_len // RATE
    far_rows = gather_far(moves, far_block)
    own = []
    for part in range(HEADS // HEADS_A_CALL):
        own.append(attend_own(part, tile_counts, slide_normed, w_query, w_key, w_value))
    core_bit = (lax.axis_index("seq") % 2).astype(jnp.int32)[None]
    attended, *parts = attend_far(
        dilated, core_bit, far_rows, w_key, w_value, grad_att, own, grad_y, slide_normed
    )
    output = slide_tok.astype(jnp.float32) + mm_tn(attended, w_out)
    slide_out = jnp.where(is_valid[:, None], output, 0.0).astype(jnp.bfloat16)
    slide_out = jnp.concatenate([slide_out, jnp.zeros((BLOCK, width), jnp.bfloat16)], axis=0)
    grad_value, grad_out = reduce_grads(moves, *parts)
    return (slide_out[None], grad_value, grad_out)


def solution(mesh):
    placed = (
        P("group", "seq", None),
        P("group", "seq"),
        P(None, ("group", "seq")),
        P(None, ("group", "seq")),
        P(None, ("group", "seq")),
        P(),
        P(),
        P(),
        P(),
        P(),
        P("group", "seq", None),
    )

    return jax.shard_map(
        shards,
        mesh=mesh,
        in_specs=placed,
        out_specs=(P("group", "seq", None), P("seq", None), P("seq", None)),
        check_vma=False,
    )
```

```python
import math

import jax
import jax.numpy as jnp
from jax import lax
from jax.experimental import pallas as pl
from jax.experimental.pallas import tpu as pltpu
from jax.sharding import PartitionSpec as P


HEADS = 16
HEAD = 48
RATE = 16
BLOCK = 32

epsilon = 1e-06
BOTH = ("group", "seq")


def rms_rows(values):
    values = values.astype(jnp.float32)
    return values * lax.rsqrt(jnp.mean(values * values, axis=-1, keepdims=True) + epsilon)


def mm(left, right):
    return jnp.dot(left, right, preferred_element_type=jnp.float32)


def mm_nt(left, right):
    return lax.dot_general(
        left, right, (((1,), (1,)), ((), ())), preferred_element_type=jnp.float32
    )


def mm_tn(left, right):
    return lax.dot_general(
        left, right, (((0,), (0,)), ((), ())), preferred_element_type=jnp.float32
    )


def project_t(weight_t, rows):
    return mm_nt(weight_t, rows).astype(jnp.bfloat16)


HEADS_A_CALL = 8
HEADS_A_STEP = 4


def valid_column(count_ref, height):
    return lax.broadcasted_iota(jnp.int32, (height, 1), 0) < count_ref[0, 0]


def grads_in_body(count_ref, cotangent_ref, w_out_ref, grad_y_ref, grad_att_ref):
    height = grad_y_ref.shape[0]
    grad_y = cotangent_ref[:height].astype(jnp.float32)
    grad_y = jnp.where(valid_column(count_ref, height), grad_y, 0.0).astype(jnp.bfloat16)
    grad_y_ref[...] = grad_y
    grad_att_ref[...] = mm_nt(w_out_ref[...], grad_y).astype(jnp.bfloat16)


def grads_in(counts, cotangent, w_out, live):
    width = w_out.shape[0]
    return pl.pallas_call(
        grads_in_body,
        in_specs=[pl.BlockSpec(memory_space=pltpu.SMEM), NEAR, NEAR],
        out_specs=[NEAR] * 2,
        out_shape=[
            pltpu.VMEM((live, width), jnp.bfloat16),
            pltpu.VMEM((width, live), jnp.bfloat16),
        ],
        compiler_params=room(8),
        name="grads_in",
    )(counts, *near(cotangent, w_out))


FAR_AWAY = pl.BlockSpec(memory_space=pltpu.HBM)


def fetch(sources, targets, sems, first=0):
    copies = []
    for i, (source, target) in enumerate(zip(sources, targets)):
        copies.append(pltpu.make_async_copy(source, target, sems.at[first + i]))
        copies[-1].start()
    return copies


def turn_body(count, *refs):
    ins, outs = refs[:count], refs[count : 2 * count]
    held, turned, sems = refs[2 * count : 3 * count], refs[3 * count : 4 * count], refs[-1]
    got = fetch(ins, held, sems)
    sent = []
    for i in range(count):
        got[i].wait()
        turned[i][...] = held[i][...].T
        sent += fetch([turned[i]], [outs[i]], sems, count + i)
    for copy in sent:
        copy.wait()


def turn(*weights):
    flat = [(w.shape[1], w.shape[0]) for w in weights]
    return pl.pallas_call(
        lambda *refs: turn_body(len(weights), *refs),
        in_specs=[FAR_AWAY] * len(weights),
        out_specs=[FAR_AWAY] * len(weights),
        out_shape=[pltpu.HBM(shape, jnp.bfloat16) for shape in flat],
        scratch_shapes=[pltpu.VMEM(w.shape, jnp.bfloat16) for w in weights]
        + [pltpu.VMEM(shape, jnp.bfloat16) for shape in flat]
        + [pltpu.SemaphoreType.DMA((2 * len(weights),))],
        compiler_params=room(16),
        name="turn",
    )(*away(*weights))


def own_body(
    part, count_ref, rows_in, wq_in, wk_in, wv_in, q_out, e_out, m_out, l_out, o_out,
    rows_ref, wq_ref, wk_ref, wv_ref, q_ref, e_ref, m_ref, l_ref, o_ref, sems,
):
    cut = pl.ds(part * HEADS_A_CALL * HEAD, HEADS_A_CALL * HEAD)
    got = fetch(
        (rows_in, wq_in.at[cut], wk_in.at[cut], wv_in.at[cut]),
        (rows_ref, wq_ref, wk_ref, wv_ref),
        sems,
    )
    got[0].wait()
    rows = rows_ref[...]
    bias = jnp.where(valid_column(count_ref, rows.shape[0]), 0.0, -1e30)
    got[1].wait()
    scale = 1.0 / (math.sqrt(HEAD) * math.log(2.0))
    q_ref[...] = (mm_nt(wq_ref[...], rows) * scale).astype(jnp.bfloat16)
    got[2].wait()
    keys = project_t(wk_ref[...], rows)
    got[3].wait()
    values = project_t(wv_ref[...], rows)
    sent = fetch([q_ref], [q_out], sems, 4)
    for h in range(HEADS_A_CALL):
        at = slice(h * HEAD, (h + 1) * HEAD)
        scores = mm_tn(keys[at], q_ref[at]) + bias
        top = jnp.max(scores, axis=0, keepdims=True)
        exponent = jnp.exp2(scores - top)
        m_ref[h] = top
        l_ref[h] = jnp.sum(exponent, axis=0, keepdims=True)
        low = exponent.astype(jnp.bfloat16)
        e_ref[h] = low
        sent += fetch([e_ref.at[h]], [e_out.at[h]], sems, 8 + h)
        o_ref[at] = mm(values[at], low)
    sent += fetch((m_ref, l_ref, o_ref), (m_out, l_out, o_out), sems, 5)
    for copy in sent:
        copy.wait()


def far_body(dilated, *refs):
    parts = HEADS // HEADS_A_CALL
    count = 6 + 5 * parts
    core_ref, ins, outs = refs[0], refs[1 : 1 + count], refs[1 + count : 6 + count]
    held, sems = refs[6 + count : 6 + 2 * count], refs[-1]
    keys_ref, values_ref, own_ref, far_ref, turned_ref, turned_far_ref = refs[-7:-1]
    got = fetch(ins, held, sems)
    rows_ref, wk_ref, wv_ref, g_ref = held[:4]
    grad_y_ref, normed_ref = held[-2:]
    att_ref = outs[0]
    got[0].wait()
    rows = rows_ref[...]
    place = lax.broadcasted_iota(jnp.int32, (dilated, 1), 0).astype(jnp.float32)
    pieces = []
    for end in range(dilated, rows.shape[0] + 1, dilated):
        pieces.append(jnp.where(place < rows_ref[end - 1 : end, :1].astype(jnp.float32), 0.0, -1e30))
    bias = jnp.concatenate(pieces, axis=0)
    got[1].wait()
    keys_ref[...] = project_t(wk_ref[...], rows)
    got[2].wait()
    values_ref[...] = project_t(wv_ref[...], rows)
    got[3].wait()

    for part in range(parts):
        for copy in got[4 + part * 5 : 9 + part * 5]:
            copy.wait()
        q_ref, e_ref, m_ref, l_ref, o_ref = held[4 + part * 5 : 9 + part * 5]
        first = part * HEADS_A_CALL * HEAD

        def step(i, _):
            for k in range(HEADS_A_STEP):
                h = i * HEADS_A_STEP + k
                here = pl.ds(pl.multiple_of(h * HEAD, HEAD), HEAD)
                at = pl.ds(pl.multiple_of(first + h * HEAD, HEAD), HEAD)
                scores = mm_tn(keys_ref[at], q_ref[here]) + bias
                top = jnp.maximum(jnp.max(scores, axis=0, keepdims=True), m_ref[h])
                ratio = jnp.exp2(m_ref[h] - top)
                exponent = jnp.exp2(scores - top)
                norm = 1.0 / (l_ref[h] * ratio + jnp.sum(exponent, axis=0, keepdims=True))
                low = exponent.astype(jnp.bfloat16)
                total = (o_ref[here] * ratio + mm(values_ref[at], low)) * norm
                att_ref[at] = total.astype(jnp.bfloat16)
                grads = g_ref[at].astype(jnp.float32) * norm
                far_ref[at] = mm_nt(grads.astype(jnp.bfloat16), low).astype(jnp.bfloat16)
                grads = (grads * ratio).astype(jnp.bfloat16)
                own_ref[at] = mm_nt(grads, e_ref[h]).astype(jnp.bfloat16)
            return 0

        lax.fori_loop(0, HEADS_A_CALL // HEADS_A_STEP, step, 0)

    share = turned_ref.shape[0] * dilated // rows.shape[0]

    def halves(ref):
        for bit in (core_ref[0], 1 - core_ref[0]):
            pieces = []
            for first in range(0, ref.shape[0], 2 * share):
                start = pl.multiple_of(first + bit * share, share)
                pieces.append(ref[pl.ds(start, share)])
            yield jnp.concatenate(pieces, axis=0)

    got[-2].wait()
    got[-1].wait()
    for half, out in zip(halves(att_ref), outs[1:3]):
        out[...] = mm(half, grad_y_ref[...]).astype(out.dtype)
    own_count = normed_ref.shape[0]
    turned_ref[:, :own_count] = normed_ref[...].T
    turned_far_ref[...] = rows.T
    for half, far, out in zip(halves(turned_ref), halves(turned_far_ref), outs[3:5]):
        total = mm_nt(half[:, :own_count], own_ref[...]) + mm_nt(far, far_ref[...])
        out[...] = total.astype(out.dtype)


def attend_own(part, counts, rows, w_query, w_key, w_value):
    count = rows.shape[0]
    features = HEADS_A_CALL * HEAD
    outs = [
        pltpu.HBM((features, count), jnp.bfloat16),
        pltpu.HBM((HEADS_A_CALL, count, count), jnp.bfloat16),
        pltpu.HBM((HEADS_A_CALL, 1, count), jnp.float32),
        pltpu.HBM((HEADS_A_CALL, 1, count), jnp.float32),
        pltpu.HBM((features, count), jnp.float32),
    ]
    cut = pltpu.VMEM((features, rows.shape[1]), jnp.bfloat16)
    return pl.pallas_call(
        lambda *refs: own_body(part, *refs),
        in_specs=[pl.BlockSpec(memory_space=pltpu.SMEM)] + [FAR_AWAY] * 4,
        out_specs=[FAR_AWAY] * 5,
        out_shape=outs,
        scratch_shapes=[
            pltpu.VMEM(rows.shape, jnp.bfloat16),
            cut,
            cut,
            cut,
        ]
        + [pltpu.VMEM(o.shape, o.dtype) for o in outs]
        + [pltpu.SemaphoreType.DMA((8 + HEADS_A_CALL,))],
        compiler_params=room(24),
        cost_estimate=pl.CostEstimate(
            flops=40 * features * count * count,
            transcendentals=HEADS_A_CALL * count * count,
            bytes_accessed=2 * HEADS_A_CALL * count * count,
        ),
        name="attend_own",
    )(counts, *away(rows, w_query, w_key, w_value))


def attend_far(dilated, core_bit, rows, w_key, w_value, grads, own, grad_y, normed):
    width, count = grads.shape
    args = [rows, w_key, w_value, grads]
    args += [array for arrays in own for array in arrays] + [grad_y, normed]
    low = jnp.bfloat16
    cut = [pltpu.VMEM((width // 2, width), jnp.float32), pltpu.VMEM((width // 2, width), low)]
    return pl.pallas_call(
        lambda *refs: far_body(dilated, *refs),
        in_specs=[pl.BlockSpec(memory_space=pltpu.SMEM)] + [FAR_AWAY] * len(args),
        out_specs=[NEAR] * 5,
        out_shape=[pltpu.VMEM((width, count), low)] + cut + cut,
        scratch_shapes=[pltpu.VMEM(a.shape, a.dtype) for a in args]
        + [pltpu.VMEM((width, rows.shape[0]), low)] * 2
        + [
            pltpu.VMEM((width, count), low),
            pltpu.VMEM((width, rows.shape[0]), low),
            pltpu.VMEM((width, count), low),
            pltpu.VMEM((width, rows.shape[0]), low),
        ]
        + [pltpu.SemaphoreType.DMA((len(args),))],
        compiler_params=room(40),
        cost_estimate=pl.CostEstimate(
            flops=40 * width * count * count,
            transcendentals=HEADS * count * count,
            bytes_accessed=2 * HEADS * count * count,
        ),
        name="attend_far",
    )(core_bit, *away(*args))


def near(*arrays):
    return tuple(pltpu.with_memory_space_constraint(a, pltpu.VMEM) for a in arrays)


def room(mebibytes):
    return pltpu.CompilerParams(vmem_limit_bytes=mebibytes << 20)


def away(*arrays):
    return tuple(pltpu.with_memory_space_constraint(a, pltpu.HBM) for a in arrays)


NEAR = pl.BlockSpec(memory_space=pltpu.VMEM)


class Moves:
    def __init__(self, groups, seqs):
        self.groups, self.seqs = groups, seqs
        self.rests = seqs // 4
        self.ring = (groups // 2) * self.rests

    def seq_xor(self, value, bit):
        return lax.ppermute(value, "seq", [(s, s ^ bit) for s in range(self.seqs)])

    def core(self, value):
        return self.seq_xor(value, 1)

    def x(self, value):
        return self.seq_xor(value, 2)

    def y(self, value):
        return lax.ppermute(value, "group", [(g, g ^ 1) for g in range(self.groups)])

    def rest_shift(self, value, step):
        pairs = []
        for s in range(self.seqs):
            target = ((s // 4 + step) % self.rests) * 4 + s % 4
            pairs.append((s, target))
        return lax.ppermute(value, "seq", pairs)

    def ring_next(self, value):
        pairs = []
        for g in range(self.groups):
            for s in range(self.seqs):
                place = ((g // 2) * self.rests + s // 4 + 1) % self.ring
                to_g = (place // self.rests) * 2 + g % 2
                to_s = (place % self.rests) * 4 + s % 4
                pairs.append((g * self.seqs + s, to_g * self.seqs + to_s))
        return lax.ppermute(value, BOTH, pairs)


def take(array, index, axis):
    return lax.dynamic_index_in_dim(array, index, axis, keepdims=False)


def ffn_term(rows, chunks, hidden):
    gate = jnp.concatenate([c[:hidden] for c in chunks], axis=0)
    upward = jnp.concatenate([c[hidden : 2 * hidden] for c in chunks], axis=0)
    down = jnp.concatenate([c[2 * hidden :] for c in chunks], axis=0)
    active = (jax.nn.silu(mm_nt(rows, gate)) * mm_nt(rows, upward)).astype(jnp.bfloat16)
    return mm(active, down)


def pack_body(gate_in, up_in, down_in, out_ref, gate_ref, up_ref, down_ref, sems):
    got = fetch((gate_in, up_in, down_in), (gate_ref, up_ref, down_ref), sems)
    for copy in got:
        copy.wait()
    hidden, width = gate_ref.shape
    lanes = 2 * hidden
    for tile in range(width // lanes):
        at = slice(tile * lanes, (tile + 1) * lanes)
        block = jnp.concatenate([gate_ref[:, at], up_ref[:, at]], axis=0)
        out_ref[at] = block.T
        out_ref[width + tile * hidden : width + (tile + 1) * hidden] = down_ref[:, at]


def pack_weights(w_gate, w_up, w_down_t):
    width, hidden = w_gate.shape
    return pl.pallas_call(
        pack_body,
        in_specs=[FAR_AWAY] * 3,
        out_specs=NEAR,
        out_shape=pltpu.VMEM((width + width // 2, 2 * hidden), jnp.bfloat16),
        scratch_shapes=[pltpu.VMEM((hidden, width), jnp.bfloat16)] * 3
        + [pltpu.SemaphoreType.DMA((3,))],
        compiler_params=room(4),
        name="pack",
    )(*away(w_gate.T, w_up.T, w_down_t.T))


def ffn_body(pieces, count, splits, *refs):
    rows_refs, chunk_refs = refs[:pieces], refs[pieces : pieces + count]
    at = pieces + count
    starts = refs[at:-splits] if len(refs) - splits > at else None
    outs = refs[-splits:]
    rows = jnp.concatenate([r[...] for r in rows_refs], axis=0)
    total = None if starts is None else jnp.concatenate([r[...] for r in starts], axis=0)
    width = rows.shape[1]
    lanes = chunk_refs[0].shape[1]
    hidden = lanes // 2
    is_low = lax.broadcasted_iota(jnp.int32, (rows.shape[0], lanes), 1) < hidden
    actives, downs = [], []
    for at in range(0, count, 2):
        pair = chunk_refs[at : at + 2]
        both = mm(rows, jnp.concatenate([c[:width] for c in pair], axis=1))
        even, odd = both[:, :lanes], both[:, lanes:]
        gate = jnp.where(is_low, even, pltpu.roll(odd, hidden, 1))
        upward = jnp.where(is_low, pltpu.roll(even, hidden, 1), odd)
        actives.append((gate / (1.0 + jnp.exp(-gate)) * upward).astype(jnp.bfloat16))
        for c in pair:
            tiles = [
                c[width + tile * hidden : width + (tile + 1) * hidden]
                for tile in range(width // lanes)
            ]
            downs.append(jnp.concatenate(tiles, axis=1))
    term = mm(jnp.concatenate(actives, axis=1), jnp.concatenate(downs, axis=0))
    total = term if total is None else total + term
    share = total.shape[0] // splits
    for i, out in enumerate(outs):
        out[...] = total[i * share : (i + 1) * share].astype(out.dtype)


def ffn_kernel(rows, chunks, starts, splits, dtype):
    width = rows[0].shape[1]
    height = sum(r.shape[0] for r in rows)
    units = len(chunks) * chunks[0].shape[1] // 2
    return pl.pallas_call(
        lambda *refs: ffn_body(len(rows), len(chunks), splits, *refs),
        in_specs=[NEAR] * (len(rows) + len(chunks) + len(starts or [])),
        out_specs=[NEAR] * splits,
        out_shape=[pltpu.VMEM((height // splits, width), dtype)] * splits,
        cost_estimate=pl.CostEstimate(
            flops=6 * height * width * units,
            transcendentals=height * units,
            bytes_accessed=2 * width * (height + 3 * units),
        ),
        compiler_params=room(24),
    )(*near(*rows, *chunks, *(starts or [])))


def norm_rows(values):
    return values * lax.rsqrt(jnp.mean(values * values, axis=-1, keepdims=True) + epsilon)


def join_body(first_ref, second_ref, out_ref):
    height = first_ref.shape[0]
    out_ref[:height] = first_ref[...]
    out_ref[height:] = second_ref[...]


def join(first, second):
    height, width = first.shape
    return pl.pallas_call(
        join_body,
        in_specs=[NEAR] * 2,
        out_specs=NEAR,
        out_shape=pltpu.VMEM((2 * height, width), first.dtype),
        compiler_params=room(2),
        name="join",
    )(*near(first, second))


def picked(rows, sources):
    at = lax.broadcasted_iota(jnp.int32, (sources.shape[0], rows.shape[0]), 1)
    return mm((at == sources).astype(jnp.bfloat16), rows)


def finish_body(count_ref, level_ref, *refs):
    sums, w_embed_ref = refs[:6], refs[6]
    slide_ref, back_ref, far_ref, far_send_ref = refs[7:]
    low = jnp.bfloat16
    mixed = []
    for kept, own, end in (sums[:3], sums[3:]):
        mixed.append(kept[...] + own[...].astype(jnp.float32) + end[...].astype(jnp.float32))
    encoded = level_ref[...].astype(jnp.float32) + jnp.concatenate(mixed, axis=0)
    slide = mm(norm_rows(encoded).astype(low), w_embed_ref[...]).astype(low)
    slide_ref[...] = slide
    half, blocks = slide.shape[0], back_ref.shape[0] // BLOCK
    for block in range(blocks):
        source = (blocks - block) * BLOCK
        back_ref[block * BLOCK : (block + 1) * BLOCK] = slide[source : source + BLOCK]
    normed = norm_rows(slide.astype(jnp.float32)).astype(low)
    place = lax.broadcasted_iota(jnp.int32, (far_ref.shape[0], 1), 0)
    own_far, sent_far = half // RATE, blocks * BLOCK // RATE
    far = picked(normed, jnp.where(place < own_far, place * RATE, -1))
    far_count = ((count_ref[0, 0] + RATE - 1) // RATE).astype(jnp.float32)
    far_ref[...] = jnp.where(place < own_far + sent_far, far, far_count).astype(low)
    step = (place - own_far) * RATE
    source = (blocks - step // BLOCK) * BLOCK + step % BLOCK
    is_sent = (place >= own_far) & (place < own_far + sent_far)
    far_send_ref[...] = picked(normed, jnp.where(is_sent, source, -1)).astype(low)


def finish(counts, level, sums, w_embed, dilated):
    half, width = level.shape[0], w_embed.shape[1]
    low = jnp.bfloat16
    return pl.pallas_call(
        finish_body,
        in_specs=[pl.BlockSpec(memory_space=pltpu.SMEM)] + [NEAR] * 8,
        out_specs=[NEAR] * 4,
        out_shape=[
            pltpu.VMEM((half, width), low),
            pltpu.VMEM((half - BLOCK, width), low),
            pltpu.VMEM((dilated, width), low),
            pltpu.VMEM((dilated, width), low),
        ],
        compiler_params=room(12),
        name="finish",
    )(counts, *near(level, *sums, w_embed))


def tokens_body(part_ref, back_ref, slide_ref, normed_ref):
    slide = jnp.concatenate([part_ref[...], back_ref[...]], axis=0)
    slide_ref[...] = slide
    normed_ref[...] = norm_rows(slide.astype(jnp.float32)).astype(jnp.bfloat16)


def tokens(part, back):
    shape = (part.shape[0] + back.shape[0], part.shape[1])
    return pl.pallas_call(
        tokens_body,
        in_specs=[NEAR] * 2,
        out_specs=[NEAR] * 2,
        out_shape=[pltpu.HBM(shape, jnp.bfloat16)] * 2,
        compiler_params=room(6),
        name="tokens",
    )(*near(part, back))


def flip_blocks(rows):
    width = rows.shape[1]
    return rows.reshape(-1, BLOCK, width)[::-1].reshape(-1, width)


def encode(moves, counts, tile_rows, row_count, w_gate, w_up, w_down_t, w_embed):
    hidden = w_gate.shape[1]
    packed = 2 * hidden == 128 and moves.ring > 1
    half = tile_rows.shape[0] // 2
    part = half // 2
    spare = half - BLOCK
    low = jnp.bfloat16
    if packed:
        chunk = pack_weights(w_gate, w_up, w_down_t)
    else:
        chunk = jnp.concatenate([w_gate.T, w_up.T, w_down_t.T], axis=0)
    ringed = [chunk]
    for _ in range(1, moves.ring):
        ringed.append(moves.ring_next(ringed[-1]))
    chunks = []
    for c in ringed:
        chunks.append([c, moves.core(c)])
    extra = flip_blocks(moves.y(tile_rows[half : half + spare]))
    own_blocks = (row_count + BLOCK - 1) // BLOCK
    kept = (1 + jnp.arange(spare) // BLOCK) < own_blocks
    level = jnp.concatenate(
        [tile_rows[:BLOCK], jnp.where(kept[:, None], tile_rows[BLOCK:half], extra)], axis=0
    )
    normed = rms_rows(level).astype(low)
    first, second = normed[:part], normed[part:]
    first = jnp.concatenate([first, moves.x(first)], axis=0)
    second = jnp.concatenate([second, moves.y(second)], axis=0)
    first_y = moves.y(first)
    second_x = moves.x(second)
    early = [c for pair in chunks[:-1] for c in pair]
    if packed:
        begun = ffn_kernel([first_y, second_x, first, second], early, None, 8, jnp.float32)
        sent = ffn_kernel([first_y, second_x], chunks[-1], begun[:4], 4, low)
        kept = ffn_kernel([first, second], chunks[-1], begun[4:], 4, jnp.float32)
    else:
        rows = jnp.concatenate([first_y, second_x, first, second], axis=0)
        mixed = ffn_term(rows, [c for pair in chunks for c in pair], hidden)
        pieces = [mixed[i * part : (i + 1) * part] for i in range(8)]
        sent, kept = [p.astype(low) for p in pieces[:4]], pieces[4:]
    first_on = moves.y(sent[1])
    second_on = moves.x(sent[3])
    first_own = moves.y(sent[0])
    second_own = moves.x(sent[2])
    first_end = moves.x((kept[1] + first_on.astype(jnp.float32)).astype(low))
    second_end = moves.y((kept[3] + second_on.astype(jnp.float32)).astype(low))
    dilated = tile_rows.shape[0] // RATE
    sums = (kept[0], first_own, first_end, kept[2], second_own, second_end)
    slide_part, to_back, far_own, far_send = finish(counts, level, sums, w_embed, dilated)
    far_got = moves.y(far_send)
    back = moves.y(to_back)
    place = jnp.arange(dilated)[:, None]
    is_got = (place >= half // RATE) & (place < (half + spare) // RATE)
    return tokens(slide_part, back), jnp.where(is_got, far_got, far_own)


def reduce_grads(moves, out_kept, out_sent, value_kept, value_sent):
    seqs = moves.seqs
    features, width = 2 * out_kept.shape[0], out_kept.shape[1]
    seq_index, group_index = lax.axis_index("seq"), lax.axis_index("group")
    x_bit, rest = (seq_index // 2) % 2, seq_index // 4
    y_bit = group_index % 2
    share = features // seqs // 2
    low = jnp.bfloat16

    def halve(array, bit, axis, move):
        kept = take(array, bit, axis).astype(jnp.float32)
        return kept + move(take(array, 1 - bit, axis).astype(low)).astype(jnp.float32)

    def with_core(kept, sent):
        total = kept + moves.core(sent).astype(jnp.float32)
        return total.reshape(moves.rests, 2, 2, share, width)

    out = with_core(out_kept, out_sent)
    value = with_core(value_kept, value_sent)
    value = halve(value, x_bit, 1, moves.x)
    out = halve(out, y_bit, 2, moves.y)
    value = halve(value, y_bit, 1, moves.y)
    out = halve(out, x_bit, 1, moves.x)
    both = jnp.concatenate([value, out], axis=2)
    total = take(both, rest, 0)
    sent = both.astype(low)
    for step in range(1, moves.rests):
        block = take(sent, (rest + step) % moves.rests, 0)
        total = total + moves.rest_shift(block, step).astype(jnp.float32)
    total = total.astype(low)
    if moves.groups > 2:
        fellows = [list(range(bit, moves.groups, 2)) for bit in range(2)]
        everyone = lax.all_gather(total, "group", axis=0, axis_index_groups=fellows)
        total = jnp.sum(everyone.astype(jnp.float32), axis=0).astype(low)
    other = moves.y(total)
    top = jnp.where(y_bit == 0, total, other)
    bottom = jnp.where(y_bit == 0, other, total)
    full = jnp.concatenate([top, bottom], axis=0).astype(jnp.float32)
    return full[:, :width], full[:, width:]


def gather_far(moves, block):
    bit = moves.seqs // 2
    while bit >= 1:
        block = join(block, moves.seq_xor(block, bit))
        bit //= 2
    return block


def shards(
    tiles, tile_counts, w_gate, w_up, w_down_t, w_embed, w_query, w_key, w_value, w_out, cotangent
):
    moves = Moves(lax.axis_size("group"), lax.axis_size("seq"))
    tile_rows = tiles[0]
    row_count = tile_counts[0, 0]
    seq_len = tile_rows.shape[0]
    live = seq_len - BLOCK
    is_valid = jnp.arange(live) < row_count
    grad_y, grad_att = grads_in(tile_counts, cotangent[0], w_out, live)
    (slide_tok, slide_normed), far_block = encode(
        moves, tile_counts, tile_rows, row_count, w_gate, w_up, w_down_t, w_embed
    )
    width = slide_tok.shape[1]
    dilated = seq_len // RATE
    far_rows = gather_far(moves, far_block)
    wq_t, wk_t, wv_t = turn(w_query, w_key, w_value)
    own = []
    for part in range(HEADS // HEADS_A_CALL):
        own.append(attend_own(part, tile_counts, slide_normed, wq_t, wk_t, wv_t))
    core_bit = (lax.axis_index("seq") % 2).astype(jnp.int32)[None]
    attended, *parts = attend_far(
        dilated, core_bit, far_rows, wk_t, wv_t, grad_att, own, grad_y, slide_normed
    )
    output = slide_tok.astype(jnp.float32) + mm_tn(attended, w_out)
    slide_out = jnp.where(is_valid[:, None], output, 0.0).astype(jnp.bfloat16)
    slide_out = jnp.concatenate([slide_out, jnp.zeros((BLOCK, width), jnp.bfloat16)], axis=0)
    grad_value, grad_out = reduce_grads(moves, *parts)
    return (slide_out[None], grad_value, grad_out)


def solution(mesh):
    placed = (
        P("group", "seq", None),
        P("group", "seq"),
        P(None, ("group", "seq")),
        P(None, ("group", "seq")),
        P(None, ("group", "seq")),
        P(),
        P(),
        P(),
        P(),
        P(),
        P("group", "seq", None),
    )

    return jax.shard_map(
        shards,
        mesh=mesh,
        in_specs=placed,
        out_specs=(P("group", "seq", None), P("seq", None), P("seq", None)),
        check_vma=False,
    )
```

```python
import math

import jax
import jax.numpy as jnp
from jax import lax
from jax.experimental import pallas as pl
from jax.experimental.pallas import tpu as pltpu
from jax.sharding import PartitionSpec as P


HEADS = 16
HEAD = 48
RATE = 16
BLOCK = 32

epsilon = 1e-06
BOTH = ("group", "seq")


def rms_rows(values):
    values = values.astype(jnp.float32)
    return values * lax.rsqrt(jnp.mean(values * values, axis=-1, keepdims=True) + epsilon)


def mm(left, right):
    return jnp.dot(left, right, preferred_element_type=jnp.float32)


def mm_nt(left, right):
    return lax.dot_general(
        left, right, (((1,), (1,)), ((), ())), preferred_element_type=jnp.float32
    )


def mm_tn(left, right):
    return lax.dot_general(
        left, right, (((0,), (0,)), ((), ())), preferred_element_type=jnp.float32
    )


def project_t(weight_t, rows):
    return mm_nt(weight_t, rows).astype(jnp.bfloat16)


HEADS_A_CALL = 8
HEADS_A_STEP = 4


def valid_column(count_ref, height):
    return lax.broadcasted_iota(jnp.int32, (height, 1), 0) < count_ref[0, 0]


def grads_in_body(count_ref, cotangent_ref, w_out_ref, grad_y_ref, grad_att_ref):
    height = grad_y_ref.shape[0]
    grad_y = cotangent_ref[:height].astype(jnp.float32)
    grad_y = jnp.where(valid_column(count_ref, height), grad_y, 0.0).astype(jnp.bfloat16)
    grad_y_ref[...] = grad_y
    grad_att_ref[...] = mm_nt(w_out_ref[...], grad_y).astype(jnp.bfloat16)


def grads_in(counts, cotangent, w_out, live):
    width = w_out.shape[0]
    return pl.pallas_call(
        grads_in_body,
        in_specs=[pl.BlockSpec(memory_space=pltpu.SMEM), NEAR, NEAR],
        out_specs=[NEAR] * 2,
        out_shape=[
            pltpu.VMEM((live, width), jnp.bfloat16),
            pltpu.VMEM((width, live), jnp.bfloat16),
        ],
        compiler_params=room(8),
        name="grads_in",
    )(counts, *near(cotangent, w_out))


FAR_AWAY = pl.BlockSpec(memory_space=pltpu.HBM)


def fetch(sources, targets, sems, first=0):
    copies = []
    for i, (source, target) in enumerate(zip(sources, targets)):
        copies.append(pltpu.make_async_copy(source, target, sems.at[first + i]))
        copies[-1].start()
    return copies


def turn_body(count, *refs):
    ins, outs = refs[:count], refs[count : 2 * count]
    held, turned, sems = refs[2 * count : 3 * count], refs[3 * count : 4 * count], refs[-1]
    got = fetch(ins, held, sems)
    sent = []
    for i in range(count):
        got[i].wait()
        turned[i][...] = held[i][...].T
        sent += fetch([turned[i]], [outs[i]], sems, count + i)
    for copy in sent:
        copy.wait()


def turn(*weights):
    flat = [(w.shape[1], w.shape[0]) for w in weights]
    return pl.pallas_call(
        lambda *refs: turn_body(len(weights), *refs),
        in_specs=[FAR_AWAY] * len(weights),
        out_specs=[FAR_AWAY] * len(weights),
        out_shape=[pltpu.HBM(shape, jnp.bfloat16) for shape in flat],
        scratch_shapes=[pltpu.VMEM(w.shape, jnp.bfloat16) for w in weights]
        + [pltpu.VMEM(shape, jnp.bfloat16) for shape in flat]
        + [pltpu.SemaphoreType.DMA((2 * len(weights),))],
        compiler_params=room(16),
        name="turn",
    )(*away(*weights))


def own_body(
    part, count_ref, rows_ref, wq_in, wk_in, wv_in, q_out, e_out, m_out, l_out, o_out,
    wq_ref, wk_ref, wv_ref, q_ref, e_ref, m_ref, l_ref, o_ref, sems,
):
    cut = pl.ds(part * HEADS_A_CALL * HEAD, HEADS_A_CALL * HEAD)
    got = fetch(
        (wq_in.at[cut], wk_in.at[cut], wv_in.at[cut]), (wq_ref, wk_ref, wv_ref), sems
    )
    rows = rows_ref[...]
    bias = jnp.where(valid_column(count_ref, rows.shape[0]), 0.0, -1e30)
    got[0].wait()
    scale = 1.0 / (math.sqrt(HEAD) * math.log(2.0))
    q_ref[...] = (mm_nt(wq_ref[...], rows) * scale).astype(jnp.bfloat16)
    got[1].wait()
    keys = project_t(wk_ref[...], rows)
    got[2].wait()
    values = project_t(wv_ref[...], rows)
    sent = fetch([q_ref], [q_out], sems, 4)
    for h in range(HEADS_A_CALL):
        at = slice(h * HEAD, (h + 1) * HEAD)
        scores = mm_tn(keys[at], q_ref[at]) + bias
        top = jnp.max(scores, axis=0, keepdims=True)
        exponent = jnp.exp2(scores - top)
        m_ref[h] = top
        l_ref[h] = jnp.sum(exponent, axis=0, keepdims=True)
        low = exponent.astype(jnp.bfloat16)
        e_ref[h] = low
        sent += fetch([e_ref.at[h]], [e_out.at[h]], sems, 8 + h)
        o_ref[at] = mm(values[at], low)
        sent += fetch([o_ref.at[at]], [o_out.at[at]], sems, 8 + HEADS_A_CALL + h)
    sent += fetch((m_ref, l_ref), (m_out, l_out), sems, 5)
    for copy in sent:
        copy.wait()


def far_body(dilated, *refs):
    parts = HEADS // HEADS_A_CALL
    count = 5 + 5 * parts
    core_ref, rows_ref = refs[:2]
    ins, outs, held = refs[2 : 2 + count], refs[2 + count : 7 + count], refs[7 + count : 7 + 2 * count]
    att_ref, keys_ref, values_ref, own_ref, far_ref, turned_ref, turned_far_ref, sems = refs[-8:]
    g_ref, grad_y_ref, normed_ref, wk_ref, wv_ref = held[-5:]
    got = {}

    def ask(*which):
        for i in which:
            got[i] = fetch([ins[i]], [held[i]], sems, i)[0]

    ask(count - 2, count - 1)
    rows = rows_ref[...]
    place = lax.broadcasted_iota(jnp.int32, (dilated, 1), 0).astype(jnp.float32)
    pieces = []
    for end in range(dilated, rows.shape[0] + 1, dilated):
        pieces.append(jnp.where(place < rows_ref[end - 1 : end, :1].astype(jnp.float32), 0.0, -1e30))
    bias = jnp.concatenate(pieces, axis=0)
    got[count - 2].wait()
    ask(*range(5), count - 5)
    keys_ref[...] = project_t(wk_ref[...], rows)
    got[count - 1].wait()
    values_ref[...] = project_t(wv_ref[...], rows)
    got[count - 5].wait()

    for part in range(parts):
        for i in range(5 * part, 5 * part + 5):
            got[i].wait()
        if part + 1 < parts:
            ask(*range(5 * part + 5, 5 * part + 10))
        else:
            ask(count - 4, count - 3)
        q_ref, e_ref, m_ref, l_ref, o_ref = held[5 * part : 5 * part + 5]
        first = part * HEADS_A_CALL * HEAD

        def step(i, _):
            for k in range(HEADS_A_STEP):
                h = i * HEADS_A_STEP + k
                here = pl.ds(pl.multiple_of(h * HEAD, HEAD), HEAD)
                at = pl.ds(pl.multiple_of(first + h * HEAD, HEAD), HEAD)
                scores = mm_tn(keys_ref[at], q_ref[here]) + bias
                top = jnp.maximum(jnp.max(scores, axis=0, keepdims=True), m_ref[h])
                ratio = jnp.exp2(m_ref[h] - top)
                exponent = jnp.exp2(scores - top)
                norm = 1.0 / (l_ref[h] * ratio + jnp.sum(exponent, axis=0, keepdims=True))
                low = exponent.astype(jnp.bfloat16)
                total = (o_ref[here] * ratio + mm(values_ref[at], low)) * norm
                att_ref[at] = total.astype(jnp.bfloat16)
                grads = g_ref[at].astype(jnp.float32) * norm
                far_ref[at] = mm_nt(grads.astype(jnp.bfloat16), low).astype(jnp.bfloat16)
                grads = (grads * ratio).astype(jnp.bfloat16)
                own_ref[at] = mm_nt(grads, e_ref[h]).astype(jnp.bfloat16)
            return 0

        lax.fori_loop(0, HEADS_A_CALL // HEADS_A_STEP, step, 0)

    share = turned_ref.shape[0] * dilated // rows.shape[0]

    def halves(ref):
        for bit in (core_ref[0], 1 - core_ref[0]):
            pieces = []
            for first in range(0, ref.shape[0], 2 * share):
                start = pl.multiple_of(first + bit * share, share)
                pieces.append(ref[pl.ds(start, share)])
            yield jnp.concatenate(pieces, axis=0)

    kept_copy = fetch([att_ref], [outs[0]], sems, count)[0]
    got[count - 4].wait()
    got[count - 3].wait()
    for half, out in zip(halves(att_ref), outs[1:3]):
        out[...] = mm(half, grad_y_ref[...]).astype(out.dtype)
    own_count = normed_ref.shape[0]
    turned_ref[:, :own_count] = normed_ref[...].T
    turned_far_ref[...] = rows.T
    for half, far, out in zip(halves(turned_ref), halves(turned_far_ref), outs[3:5]):
        total = mm_nt(half[:, :own_count], own_ref[...]) + mm_nt(far, far_ref[...])
        out[...] = total.astype(out.dtype)
    kept_copy.wait()


def attend_own(part, counts, rows, w_query, w_key, w_value):
    count = rows.shape[0]
    features = HEADS_A_CALL * HEAD
    outs = [
        pltpu.HBM((features, count), jnp.bfloat16),
        pltpu.HBM((HEADS_A_CALL, count, count), jnp.bfloat16),
        pltpu.HBM((HEADS_A_CALL, 1, count), jnp.float32),
        pltpu.HBM((HEADS_A_CALL, 1, count), jnp.float32),
        pltpu.HBM((features, count), jnp.float32),
    ]
    cut = pltpu.VMEM((features, rows.shape[1]), jnp.bfloat16)
    return pl.pallas_call(
        lambda *refs: own_body(part, *refs),
        in_specs=[pl.BlockSpec(memory_space=pltpu.SMEM), NEAR] + [FAR_AWAY] * 3,
        out_specs=[FAR_AWAY] * 5,
        out_shape=outs,
        scratch_shapes=[
            cut,
            cut,
            cut,
        ]
        + [pltpu.VMEM(o.shape, o.dtype) for o in outs]
        + [pltpu.SemaphoreType.DMA((8 + 2 * HEADS_A_CALL,))],
        compiler_params=room(24),
        cost_estimate=pl.CostEstimate(
            flops=40 * features * count * count,
            transcendentals=HEADS_A_CALL * count * count,
            bytes_accessed=2 * HEADS_A_CALL * count * count,
        ),
        name="attend_own",
    )(counts, *near(rows), *away(w_query, w_key, w_value))


def attend_far(dilated, core_bit, rows, w_key, w_value, grads, own, grad_y, normed):
    width, count = grads.shape
    args = [array for arrays in own for array in arrays]
    args += [grads, grad_y, normed, w_key, w_value]
    low = jnp.bfloat16
    cut = [pltpu.VMEM((width // 2, width), jnp.float32), pltpu.VMEM((width // 2, width), low)]
    return pl.pallas_call(
        lambda *refs: far_body(dilated, *refs),
        in_specs=[pl.BlockSpec(memory_space=pltpu.SMEM)] + [NEAR] + [FAR_AWAY] * len(args),
        out_specs=[FAR_AWAY] + [NEAR] * 4,
        out_shape=[pltpu.HBM((width, count), low)] + cut + cut,
        scratch_shapes=[pltpu.VMEM(a.shape, a.dtype) for a in args]
        + [pltpu.VMEM((width, count), low)]
        + [pltpu.VMEM((width, rows.shape[0]), low)] * 2
        + [
            pltpu.VMEM((width, count), low),
            pltpu.VMEM((width, rows.shape[0]), low),
            pltpu.VMEM((width, count), low),
            pltpu.VMEM((width, rows.shape[0]), low),
        ]
        + [pltpu.SemaphoreType.DMA((len(args) + 1,))],
        compiler_params=room(40),
        cost_estimate=pl.CostEstimate(
            flops=40 * width * count * count,
            transcendentals=HEADS * count * count,
            bytes_accessed=2 * HEADS * count * count,
        ),
        name="attend_far",
    )(core_bit, *near(rows), *away(*args))


def near(*arrays):
    return tuple(pltpu.with_memory_space_constraint(a, pltpu.VMEM) for a in arrays)


def room(mebibytes):
    return pltpu.CompilerParams(vmem_limit_bytes=mebibytes << 20)


def away(*arrays):
    return tuple(pltpu.with_memory_space_constraint(a, pltpu.HBM) for a in arrays)


NEAR = pl.BlockSpec(memory_space=pltpu.VMEM)


class Moves:
    def __init__(self, groups, seqs):
        self.groups, self.seqs = groups, seqs
        self.rests = seqs // 4
        self.ring = (groups // 2) * self.rests

    def seq_xor(self, value, bit):
        return lax.ppermute(value, "seq", [(s, s ^ bit) for s in range(self.seqs)])

    def core(self, value):
        return self.seq_xor(value, 1)

    def x(self, value):
        return self.seq_xor(value, 2)

    def y(self, value):
        return lax.ppermute(value, "group", [(g, g ^ 1) for g in range(self.groups)])

    def rest_shift(self, value, step):
        pairs = []
        for s in range(self.seqs):
            target = ((s // 4 + step) % self.rests) * 4 + s % 4
            pairs.append((s, target))
        return lax.ppermute(value, "seq", pairs)

    def ring_next(self, value):
        order = [0, *range(1, self.ring, 2), *range((self.ring - 1) // 2 * 2, 0, -2)]
        after = {place: order[(i + 1) % self.ring] for i, place in enumerate(order)}
        pairs = []
        for g in range(self.groups):
            for s in range(self.seqs):
                place = after[(g // 2) * self.rests + s // 4]
                to_g = (place // self.rests) * 2 + g % 2
                to_s = (place % self.rests) * 4 + s % 4
                pairs.append((g * self.seqs + s, to_g * self.seqs + to_s))
        return lax.ppermute(value, BOTH, pairs)


def take(array, index, axis):
    return lax.dynamic_index_in_dim(array, index, axis, keepdims=False)


def ffn_term(rows, chunks, hidden):
    gate = jnp.concatenate([c[:hidden] for c in chunks], axis=0)
    upward = jnp.concatenate([c[hidden : 2 * hidden] for c in chunks], axis=0)
    down = jnp.concatenate([c[2 * hidden :] for c in chunks], axis=0)
    active = (jax.nn.silu(mm_nt(rows, gate)) * mm_nt(rows, upward)).astype(jnp.bfloat16)
    return mm(active, down)


def pack_body(gate_in, up_in, down_in, out_ref, gate_ref, up_ref, down_ref, sems):
    got = fetch((gate_in, up_in, down_in), (gate_ref, up_ref, down_ref), sems)
    for copy in got:
        copy.wait()
    hidden, width = gate_ref.shape
    lanes = 2 * hidden
    for tile in range(width // lanes):
        at = slice(tile * lanes, (tile + 1) * lanes)
        block = jnp.concatenate([gate_ref[:, at], up_ref[:, at]], axis=0)
        out_ref[at] = block.T
        out_ref[width + tile * hidden : width + (tile + 1) * hidden] = down_ref[:, at]


def pack_weights(w_gate, w_up, w_down_t):
    width, hidden = w_gate.shape
    return pl.pallas_call(
        pack_body,
        in_specs=[FAR_AWAY] * 3,
        out_specs=NEAR,
        out_shape=pltpu.VMEM((width + width // 2, 2 * hidden), jnp.bfloat16),
        scratch_shapes=[pltpu.VMEM((hidden, width), jnp.bfloat16)] * 3
        + [pltpu.SemaphoreType.DMA((3,))],
        compiler_params=room(4),
        name="pack",
    )(*away(w_gate.T, w_up.T, w_down_t.T))


def ffn_body(pieces, count, splits, *refs):
    rows_refs, chunk_refs = refs[:pieces], refs[pieces : pieces + count]
    at = pieces + count
    starts = refs[at:-splits] if len(refs) - splits > at else None
    outs = refs[-splits:]
    rows = jnp.concatenate([r[...] for r in rows_refs], axis=0)
    total = None if starts is None else jnp.concatenate([r[...] for r in starts], axis=0)
    width = rows.shape[1]
    lanes = chunk_refs[0].shape[1]
    hidden = lanes // 2
    is_low = lax.broadcasted_iota(jnp.int32, (rows.shape[0], lanes), 1) < hidden
    actives, downs = [], []
    for at in range(0, count, 2):
        pair = chunk_refs[at : at + 2]
        both = mm(rows, jnp.concatenate([c[:width] for c in pair], axis=1))
        even, odd = both[:, :lanes], both[:, lanes:]
        gate = jnp.where(is_low, even, pltpu.roll(odd, hidden, 1))
        upward = jnp.where(is_low, pltpu.roll(even, hidden, 1), odd)
        actives.append((gate / (1.0 + jnp.exp(-gate)) * upward).astype(jnp.bfloat16))
        for c in pair:
            tiles = [
                c[width + tile * hidden : width + (tile + 1) * hidden]
                for tile in range(width // lanes)
            ]
            downs.append(jnp.concatenate(tiles, axis=1))
    term = mm(jnp.concatenate(actives, axis=1), jnp.concatenate(downs, axis=0))
    total = term if total is None else total + term
    share = total.shape[0] // splits
    for i, out in enumerate(outs):
        out[...] = total[i * share : (i + 1) * share].astype(out.dtype)


def ffn_kernel(rows, chunks, starts, splits, dtype):
    width = rows[0].shape[1]
    height = sum(r.shape[0] for r in rows)
    units = len(chunks) * chunks[0].shape[1] // 2
    return pl.pallas_call(
        lambda *refs: ffn_body(len(rows), len(chunks), splits, *refs),
        in_specs=[NEAR] * (len(rows) + len(chunks) + len(starts or [])),
        out_specs=[NEAR] * splits,
        out_shape=[pltpu.VMEM((height // splits, width), dtype)] * splits,
        cost_estimate=pl.CostEstimate(
            flops=6 * height * width * units,
            transcendentals=height * units,
            bytes_accessed=2 * width * (height + 3 * units),
        ),
        compiler_params=room(24),
    )(*near(*rows, *chunks, *(starts or [])))


def norm_rows(values):
    return values * lax.rsqrt(jnp.mean(values * values, axis=-1, keepdims=True) + epsilon)


def join_body(first_ref, second_ref, out_ref):
    height = first_ref.shape[0]
    out_ref[:height] = first_ref[...]
    out_ref[height:] = second_ref[...]


def join(first, second):
    height, width = first.shape
    return pl.pallas_call(
        join_body,
        in_specs=[NEAR] * 2,
        out_specs=NEAR,
        out_shape=pltpu.VMEM((2 * height, width), first.dtype),
        compiler_params=room(2),
        name="join",
    )(*near(first, second))


def picked(rows, sources):
    at = lax.broadcasted_iota(jnp.int32, (sources.shape[0], rows.shape[0]), 1)
    return mm((at == sources).astype(jnp.bfloat16), rows)


def finish_body(count_ref, level_ref, *refs):
    sums, w_embed_ref = refs[:6], refs[6]
    slide_ref, back_ref, far_ref, far_send_ref = refs[7:]
    low = jnp.bfloat16
    mixed = []
    for kept, own, end in (sums[:3], sums[3:]):
        mixed.append(kept[...] + own[...].astype(jnp.float32) + end[...].astype(jnp.float32))
    encoded = level_ref[...].astype(jnp.float32) + jnp.concatenate(mixed, axis=0)
    slide = mm(norm_rows(encoded).astype(low), w_embed_ref[...]).astype(low)
    slide_ref[...] = slide
    half, blocks = slide.shape[0], back_ref.shape[0] // BLOCK
    for block in range(blocks):
        source = (blocks - block) * BLOCK
        back_ref[block * BLOCK : (block + 1) * BLOCK] = slide[source : source + BLOCK]
    normed = norm_rows(slide.astype(jnp.float32)).astype(low)
    place = lax.broadcasted_iota(jnp.int32, (far_ref.shape[0], 1), 0)
    own_far, sent_far = half // RATE, blocks * BLOCK // RATE
    far = picked(normed, jnp.where(place < own_far, place * RATE, -1))
    far_count = ((count_ref[0, 0] + RATE - 1) // RATE).astype(jnp.float32)
    far_ref[...] = jnp.where(place < own_far + sent_far, far, far_count).astype(low)
    step = (place - own_far) * RATE
    source = (blocks - step // BLOCK) * BLOCK + step % BLOCK
    is_sent = (place >= own_far) & (place < own_far + sent_far)
    far_send_ref[...] = picked(normed, jnp.where(is_sent, source, -1)).astype(low)


def finish(counts, level, sums, w_embed, dilated):
    half, width = level.shape[0], w_embed.shape[1]
    low = jnp.bfloat16
    return pl.pallas_call(
        finish_body,
        in_specs=[pl.BlockSpec(memory_space=pltpu.SMEM)] + [NEAR] * 8,
        out_specs=[NEAR] * 4,
        out_shape=[
            pltpu.VMEM((half, width), low),
            pltpu.VMEM((half - BLOCK, width), low),
            pltpu.VMEM((dilated, width), low),
            pltpu.VMEM((dilated, width), low),
        ],
        compiler_params=room(12),
        name="finish",
    )(counts, *near(level, *sums, w_embed))


def tokens_body(part_ref, back_ref, slide_ref, normed_ref, near_ref):
    slide = jnp.concatenate([part_ref[...], back_ref[...]], axis=0)
    slide_ref[...] = slide
    normed = norm_rows(slide.astype(jnp.float32)).astype(jnp.bfloat16)
    normed_ref[...] = normed
    near_ref[...] = normed


def tokens(part, back):
    shape = (part.shape[0] + back.shape[0], part.shape[1])
    return pl.pallas_call(
        tokens_body,
        in_specs=[NEAR] * 2,
        out_specs=[NEAR] * 3,
        out_shape=[pltpu.HBM(shape, jnp.bfloat16)] * 2 + [pltpu.VMEM(shape, jnp.bfloat16)],
        compiler_params=room(6),
        name="tokens",
    )(*near(part, back))


def flip_blocks(rows):
    width = rows.shape[1]
    return rows.reshape(-1, BLOCK, width)[::-1].reshape(-1, width)


def encode(moves, counts, tile_rows, row_count, w_gate, w_up, w_down_t, w_embed):
    hidden = w_gate.shape[1]
    packed = 2 * hidden == 128 and moves.ring > 1
    half = tile_rows.shape[0] // 2
    part = half // 2
    spare = half - BLOCK
    low = jnp.bfloat16
    if packed:
        chunk = pack_weights(w_gate, w_up, w_down_t)
    else:
        chunk = jnp.concatenate([w_gate.T, w_up.T, w_down_t.T], axis=0)
    ringed = [chunk]
    for _ in range(1, moves.ring):
        ringed.append(moves.ring_next(ringed[-1]))
    chunks = []
    for c in ringed:
        chunks.append([c, moves.core(c)])
    extra = flip_blocks(moves.y(tile_rows[half : half + spare]))
    own_blocks = (row_count + BLOCK - 1) // BLOCK
    kept = (1 + jnp.arange(spare) // BLOCK) < own_blocks
    level = jnp.concatenate(
        [tile_rows[:BLOCK], jnp.where(kept[:, None], tile_rows[BLOCK:half], extra)], axis=0
    )
    normed = rms_rows(level).astype(low)
    first, second = normed[:part], normed[part:]
    first = jnp.concatenate([first, moves.x(first)], axis=0)
    second = jnp.concatenate([second, moves.y(second)], axis=0)
    first_y = moves.y(first)
    second_x = moves.x(second)
    early = [c for pair in chunks[:-1] for c in pair]
    if packed:
        begun = ffn_kernel([first_y, second_x, first, second], early, None, 8, jnp.float32)
        sent = ffn_kernel([first_y, second_x], chunks[-1], begun[:4], 4, low)
        kept = ffn_kernel([first, second], chunks[-1], begun[4:], 4, jnp.float32)
    else:
        rows = jnp.concatenate([first_y, second_x, first, second], axis=0)
        mixed = ffn_term(rows, [c for pair in chunks for c in pair], hidden)
        pieces = [mixed[i * part : (i + 1) * part] for i in range(8)]
        sent, kept = [p.astype(low) for p in pieces[:4]], pieces[4:]
    first_on = moves.y(sent[1])
    second_on = moves.x(sent[3])
    first_own = moves.y(sent[0])
    second_own = moves.x(sent[2])
    first_end = moves.x((kept[1] + first_on.astype(jnp.float32)).astype(low))
    second_end = moves.y((kept[3] + second_on.astype(jnp.float32)).astype(low))
    dilated = tile_rows.shape[0] // RATE
    sums = (kept[0], first_own, first_end, kept[2], second_own, second_end)
    slide_part, to_back, far_own, far_send = finish(counts, level, sums, w_embed, dilated)
    far_got = moves.y(far_send)
    back = moves.y(to_back)
    place = jnp.arange(dilated)[:, None]
    is_got = (place >= half // RATE) & (place < (half + spare) // RATE)
    return tokens(slide_part, back), jnp.where(is_got, far_got, far_own)


def reduce_grads(moves, out_kept, out_sent, value_kept, value_sent):
    seqs = moves.seqs
    features, width = 2 * out_kept.shape[0], out_kept.shape[1]
    seq_index, group_index = lax.axis_index("seq"), lax.axis_index("group")
    x_bit, rest = (seq_index // 2) % 2, seq_index // 4
    y_bit = group_index % 2
    share = features // seqs // 2
    low = jnp.bfloat16

    def halve(array, bit, axis, move):
        kept = take(array, bit, axis).astype(jnp.float32)
        return kept + move(take(array, 1 - bit, axis).astype(low)).astype(jnp.float32)

    def with_core(kept, sent):
        total = kept + moves.core(sent).astype(jnp.float32)
        return total.reshape(moves.rests, 2, 2, share, width)

    out = with_core(out_kept, out_sent)
    value = with_core(value_kept, value_sent)
    value = halve(value, x_bit, 1, moves.x)
    out = halve(out, y_bit, 2, moves.y)
    value = halve(value, y_bit, 1, moves.y)
    out = halve(out, x_bit, 1, moves.x)
    both = jnp.concatenate([value, out], axis=2)
    total = take(both, rest, 0)
    sent = both.astype(low)
    for step in range(1, moves.rests):
        block = take(sent, (rest + step) % moves.rests, 0)
        total = total + moves.rest_shift(block, step).astype(jnp.float32)
    total = total.astype(low)
    if moves.groups > 2:
        fellows = [list(range(bit, moves.groups, 2)) for bit in range(2)]
        everyone = lax.all_gather(total, "group", axis=0, axis_index_groups=fellows)
        total = jnp.sum(everyone.astype(jnp.float32), axis=0).astype(low)
    other = moves.y(total)
    top = jnp.where(y_bit == 0, total, other)
    bottom = jnp.where(y_bit == 0, other, total)
    full = jnp.concatenate([top, bottom], axis=0).astype(jnp.float32)
    return full[:, :width], full[:, width:]


def gather_far(moves, block):
    bit = moves.seqs // 2
    while bit >= 1:
        block = join(block, moves.seq_xor(block, bit))
        bit //= 2
    return block


def shards(
    tiles, tile_counts, w_gate, w_up, w_down_t, w_embed, w_query, w_key, w_value, w_out, cotangent
):
    moves = Moves(lax.axis_size("group"), lax.axis_size("seq"))
    tile_rows = tiles[0]
    row_count = tile_counts[0, 0]
    seq_len = tile_rows.shape[0]
    live = seq_len - BLOCK
    is_valid = jnp.arange(live) < row_count
    grad_y, grad_att = grads_in(tile_counts, cotangent[0], w_out, live)
    (slide_tok, slide_normed, near_normed), far_block = encode(
        moves, tile_counts, tile_rows, row_count, w_gate, w_up, w_down_t, w_embed
    )
    width = slide_tok.shape[1]
    dilated = seq_len // RATE
    far_rows = gather_far(moves, far_block)
    wq_t, wk_t, wv_t = turn(w_query, w_key, w_value)
    own = []
    for part in range(HEADS // HEADS_A_CALL):
        own.append(attend_own(part, tile_counts, near_normed, wq_t, wk_t, wv_t))
    core_bit = (lax.axis_index("seq") % 2).astype(jnp.int32)[None]
    attended, *parts = attend_far(
        dilated, core_bit, far_rows, wk_t, wv_t, grad_att, own, grad_y, slide_normed
    )
    output = slide_tok.astype(jnp.float32) + mm_tn(attended, w_out)
    slide_out = jnp.where(is_valid[:, None], output, 0.0).astype(jnp.bfloat16)
    slide_out = jnp.concatenate([slide_out, jnp.zeros((BLOCK, width), jnp.bfloat16)], axis=0)
    grad_value, grad_out = reduce_grads(moves, *parts)
    return (slide_out[None], grad_value, grad_out)


def solution(mesh):
    placed = (
        P("group", "seq", None),
        P("group", "seq"),
        P(None, ("group", "seq")),
        P(None, ("group", "seq")),
        P(None, ("group", "seq")),
        P(),
        P(),
        P(),
        P(),
        P(),
        P("group", "seq", None),
    )

    return jax.shard_map(
        shards,
        mesh=mesh,
        in_specs=placed,
        out_specs=(P("group", "seq", None), P("seq", None), P("seq", None)),
        check_vma=False,
    )
```
